512 devices in a mesh: dom: 64 (over z, y), feat: 8 (over x, core).
Axes of the slice: x: 4, y: 8, z: 8, core: 2. Of those that a mesh axis runs over, the one named last changes fastest.
Arguments:
- features: bfloat16 [131072, 608], P('dom', 'feat'), may hold values from -6 to 6
- weight: bfloat16 [608, 256], replicated, may hold values from -0.25 to 0.25
- out_bias: float32 [256], P('feat'), may hold values from -3 to 3
- tile_values: bfloat16 [6912, 128, 128], P('dom'), may hold values from -0.25 to 0.25
- tile_rows: int32 [6912], P('dom'), may hold values from 0 to 15
- tile_cols: int32 [6912], P('dom'), may hold values from 0 to 87, as said below
- tile_count: int32 [64], P('dom'), may hold values from 10 to 108, as said below
- send_rows: int32 [64, 8, 1024], P('dom'), may hold values from 0 to 2047
- hub_ids: int32 [1024], replicated, may hold values from 0 to 131071, as said below
Outputs:
- activations: bfloat16 [131072, 256], P('dom', 'feat')
The draws below stay inside these ranges and needn't reach their ends.
Inputs may be any that keep to these rules, and one draw needn't show every extreme that they name: `tile_count`: slots at or past a partition's count are not part of the graph; some partition uses all 108 slots. `tile_cols`: column blocks index the extended row space of the slot's partition. `hub_ids`: distinct vertex ids; vertex v belongs to partition v // 2048; no partition owns more than 48 hubs, and some partition owns exactly 48.
All inputs are finite; a program needn't handle non-finite values.
Results may differ from the reference program's by a relative error of at most 0.0044.
Values may be sent and summed in bfloat16 or wider, within the bound.
A program may use at most 64 MiB of HBM per device.

```python
import jax
import jax.numpy as jnp
from jax import lax

F_IN = 608
HID = 256
BLK = 128
VDEV = 2048
REACH = 4
HUB_MOST = 48
TILE_MOST = 108
HALO = 1024
HUBS = 1024
EXT = 11264
VERTICES = 131072
PARTITIONS = 64
TILES = 6912
N_DOM = 64


def draw_tile_count(key, part):
    lowest = 2 * REACH + 2
    spread = TILE_MOST - lowest + 1
    key_list = jax.random.split(jax.random.fold_in(key, 11), 2)
    raw_draws = jax.random.randint(key_list[0], (N_DOM,), 0, spread)
    counts = lowest + raw_draws * raw_draws // spread
    fullest = jax.random.randint(key_list[1], (), 0, N_DOM)
    counts = jnp.where(jnp.arange(N_DOM) == fullest, TILE_MOST, counts)
    return counts.astype(jnp.int32)


def draw_tile_cols(key, part):
    block_total = ((1 + REACH) * VDEV + HUBS) // BLK
    hub_first = (1 + REACH) * VDEV // BLK
    key_list = jax.random.split(jax.random.fold_in(key, 23), 3)
    columns = jax.random.randint(key_list[0], (N_DOM, TILE_MOST), 0, block_total)
    position = jnp.arange(TILE_MOST)[None, :]
    segment_start = (VDEV + position * (VDEV // 2)) // BLK
    hub_pick = jax.random.randint(key_list[1], (N_DOM, 1), hub_first, block_total)
    local_pick = jax.random.randint(key_list[2], (N_DOM, 1), 0, VDEV // BLK)
    columns = jnp.where(position < 2 * REACH, segment_start, columns)
    columns = jnp.where(position == 2 * REACH, hub_pick, columns)
    columns = jnp.where(position == 2 * REACH + 1, local_pick, columns)
    return columns.reshape(N_DOM * TILE_MOST).astype(jnp.int32)


def draw_hub_ids(key, part):
    key_list = jax.random.split(jax.random.fold_in(key, 37), 4)
    slot_total = N_DOM * HUB_MOST
    positions = jnp.arange(slot_total)
    owners = positions // HUB_MOST
    ranks = positions % HUB_MOST
    device_level = jax.random.randint(key_list[0], (N_DOM,), 0, 4)
    fullest = jax.random.randint(key_list[1], (), 0, N_DOM)
    jitter = jax.random.randint(key_list[2], (slot_total,), 0, 1024)
    scores = (device_level[owners] * 1024 + jitter) * slot_total + positions
    scores = jnp.where(owners == fullest, scores + 8 * 1024 * slot_total, scores)
    chosen = jax.lax.top_k(scores.astype(jnp.int32), HUBS)[1]
    stride = VDEV // HUB_MOST
    shifts = jax.random.randint(key_list[3], (N_DOM,), 0, stride)
    chosen_owner = owners[chosen]
    local_rows = ranks[chosen] * stride + shifts[chosen_owner]
    return (chosen_owner * VDEV + local_rows).astype(jnp.int32)


def with_ends(drawn, own_key, smallest, largest):
    longest = drawn.shape.index(max(drawn.shape))
    spots = []
    for shift in (0, 1):
        where = [jax.random.randint(jax.random.fold_in(own_key, axis), (), 0, length) for axis, length in enumerate(drawn.shape)]
        where[longest] = (where[longest] + shift) % drawn.shape[longest]
        spots.append(tuple(where))
    return drawn.at[spots[0]].set(smallest).at[spots[1]].set(largest)


def block_levels(own_key, shape, cuts, low, top_value):
    level, own = 1.0, jax.random.fold_in(own_key, 6)
    for dim, blocks in cuts:
        draws = jnp.exp(jax.random.uniform(jax.random.fold_in(own, dim), (blocks,), jnp.float32, low / len(cuts), top_value / len(cuts)))
        level = level * jnp.repeat(draws, shape[dim] // blocks).reshape([-1 if axis == dim else 1 for axis in range(len(shape))])
    return level


def bell_draw(rng, extent, scale, bound, cuts=(), kind=jnp.bfloat16):
    values = jax.random.normal(rng, extent, jnp.float32) * scale
    if len(cuts) > 0:
        values = block_levels(rng, extent, cuts, -0.22, 0.18) * values
    return jnp.clip(values, min=-bound, max=bound).astype(kind)


def setup_inputs(seed: int = 0) -> dict:
    seeds = jax.random.split(jax.random.key(seed), 10)
    features = bell_draw(seeds[0], (VERTICES, F_IN), 1.0, 6.0, ((0, 64), (1, 8)))
    weight = bell_draw(seeds[1], (F_IN, HID), F_IN ** -0.5, 0.25)
    out_bias = bell_draw(seeds[2], (HID,), 0.5, 3.0, ((0, 8),), jnp.float32)
    tile_values = bell_draw(seeds[3], (TILES, BLK, BLK), (4 * BLK) ** -0.5, 0.25, ((0, 64),))
    tile_rows = with_ends(jax.random.randint(seeds[4], (TILES,), 0, VDEV // BLK), jax.random.fold_in(seeds[4], 1), 0, (VDEV // BLK) - 1).astype(jnp.int32)
    tile_cols = draw_tile_cols(jax.random.fold_in(seeds[9], 71), 0)
    tile_count = draw_tile_count(jax.random.fold_in(seeds[9], 71), 0)
    send_rows = with_ends(jax.random.randint(seeds[7], (PARTITIONS, 2 * REACH, HALO), 0, VDEV), jax.random.fold_in(seeds[7], 1), 0, VDEV - 1).astype(jnp.int32)
    hub_ids = draw_hub_ids(jax.random.fold_in(seeds[9], 71), 0)
    return {"features": features, "weight": weight, "out_bias": out_bias, "tile_values": tile_values, "tile_rows": tile_rows, "tile_cols": tile_cols, "tile_count": tile_count, "send_rows": send_rows, "hub_ids": hub_ids}


def reference(features, weight, out_bias, tile_values, tile_rows, tile_cols, tile_count, send_rows, hub_ids):
    projected = jnp.dot(features, weight, preferred_element_type=jnp.float32).astype(jnp.bfloat16)
    hub_rows = projected[hub_ids]
    offsets = jnp.array(list(range(-REACH, 0)) + list(range(1, REACH + 1)), jnp.int32)
    slot_ids = jnp.arange(2 * REACH).astype(jnp.int32)

    def one_partition(partition):
        own_rows = lax.dynamic_slice_in_dim(projected, partition * VDEV, VDEV, 0)
        sources = partition - offsets
        present = (sources >= 0) & (sources < N_DOM)
        clipped = jnp.clip(sources, 0, N_DOM - 1).astype(jnp.int32)
        listed = send_rows[clipped, slot_ids]
        picked = projected[clipped[:, None] * VDEV + listed]
        picked = jnp.where(present[:, None, None], picked, jnp.zeros_like(picked))
        extended = jnp.concatenate([own_rows, picked.reshape(REACH * VDEV, HID), hub_rows], 0)
        blocks = extended.reshape(EXT // BLK, BLK, HID)
        col_blocks = lax.dynamic_slice_in_dim(tile_cols, partition * TILE_MOST, TILE_MOST, 0)
        row_blocks = lax.dynamic_slice_in_dim(tile_rows, partition * TILE_MOST, TILE_MOST, 0)
        own_tiles = lax.dynamic_slice_in_dim(tile_values, partition * TILE_MOST, TILE_MOST, 0)
        products = jnp.einsum("tij,tjc->tic", own_tiles.astype(jnp.float32), blocks[col_blocks].astype(jnp.float32), precision=lax.Precision.HIGHEST)
        live_mask = jnp.arange(TILE_MOST).astype(jnp.int32) < tile_count[partition]
        products = jnp.where(live_mask[:, None, None], products, jnp.zeros_like(products))
        aggregate = jax.ops.segment_sum(products, row_blocks, num_segments=VDEV // BLK)
        return jnp.maximum(aggregate.reshape(VDEV, HID) + out_bias, 0.0).astype(jnp.bfloat16)

    result = lax.map(one_partition, jnp.arange(N_DOM, dtype=jnp.int32))
    return result.reshape(N_DOM * VDEV, HID)
```

```python
import functools

import jax
import jax.numpy as jnp
from jax import lax
from jax.experimental import pallas as pl
from jax.experimental.pallas import tpu as pltpu
from jax.sharding import PartitionSpec as P

REACH = 4
HUB_MOST = 48
Y_RING = 8
LO = 256
BLK = 128
OFFSETS = tuple(range(-REACH, 0)) + tuple(range(1, REACH + 1))
SEND_ORDER = (0, 7, 1, 6, 2, 5, 3, 4)
MESH = pl.DeviceIdType.MESH
F32, BF16, I32 = jnp.float32, jnp.bfloat16, jnp.int32


def dims(a, b):
    return (((a,), (b,)), ((), ()))


def dot(a, b, ca=1, cb=0):
    return lax.dot_general(a, b, dims(ca, cb), preferred_element_type=F32)


def ones_where(mask):
    return jnp.where(mask, 1.0, 0.0).astype(BF16)


def pick_groups(stacked, group_of, groups, height):
    total = None
    for g in range(groups):
        part = jnp.where(group_of == g, stacked[g * height : (g + 1) * height], 0.0)
        total = part if total is None else total + part
    return total


def exchange_kernel(
    n_dom, n_feat, cols, chunk,
    ft_ref, w_ref, send_ref, hub_ref, ext_ref,
    part_ref, hot_ref, hubhot_ref, endhot_ref, sx, rx, sy, hub_out, hy, hpack, hz,
    sxs, sxr, sys_, syr, hys, hyr, hzs, hzr,
):
    p = lax.axis_index("dom")
    j = lax.axis_index("feat")
    y = lax.rem(p, Y_RING)
    z = lax.div(p, Y_RING)
    z_ring = n_dom // Y_RING
    k_in, rows = ft_ref.shape
    hid = w_ref.shape[1]
    n_chunk = cols // chunk
    his = rows // LO
    halo = send_ref.shape[1]
    own_blocks = rows // BLK
    slot_blocks = halo // BLK
    hub_first = own_blocks + len(OFFSETS) * slot_blocks

    def dom_at(step):
        return lax.rem(p + step + n_dom, n_dom)

    def y_at(step):
        return z * Y_RING + lax.rem(y + step, Y_RING)

    def z_at(step):
        return lax.rem(z + step, z_ring) * Y_RING + y

    def feat_at(step):
        return lax.rem(j + step, n_feat)

    barrier = pltpu.get_barrier_semaphore()
    greeted = 0
    for d in range(1, n_feat):
        pl.semaphore_signal(barrier, inc=1, device_id={"feat": feat_at(d)}, device_id_type=MESH)
        greeted += 1
    for o in OFFSETS:
        pl.semaphore_signal(barrier, inc=1, device_id={"dom": dom_at(o)}, device_id_type=MESH)
        greeted += 1
    for d in range(1, Y_RING):
        pl.semaphore_signal(barrier, inc=1, device_id={"dom": y_at(d)}, device_id_type=MESH)
        greeted += 1
    for d in range(1, z_ring):
        pl.semaphore_signal(barrier, inc=1, device_id={"dom": z_at(d)}, device_id_type=MESH)
        greeted += 1

    f_in = w_ref.shape[0]
    pick = ones_where(
        lax.broadcasted_iota(I32, (BLK, f_in), 1)
        == lax.broadcasted_iota(I32, (BLK, f_in), 0) + j * k_in
    )
    w_mine = dot(pick, w_ref[...])
    w_t = w_mine.T.astype(BF16)[:, :k_in]
    ft = ft_ref[...]

    def partials(h):
        left = jnp.concatenate(
            [w_t[d * cols + h * chunk : d * cols + (h + 1) * chunk] for d in range(n_feat)], 0
        )
        part = dot(left, ft)
        for d in range(n_feat):
            block = part[d * chunk : (d + 1) * chunk]
            part_ref[d, h * chunk : (h + 1) * chunk, :] = block
            sx[d, h] = block.astype(BF16)

    for h in range(n_chunk):
        partials(h)

    pl.semaphore_wait(barrier, greeted)

    x_copies = {}
    for h in range(n_chunk):
        for d in range(1, n_feat):
            x_copies[h, d] = pltpu.make_async_remote_copy(
                src_ref=sx.at[feat_at(d), h],
                dst_ref=rx.at[h, d - 1],
                send_sem=sxs.at[h, d - 1],
                recv_sem=sxr.at[h, d - 1],
                device_id={"feat": feat_at(d)},
                device_id_type=MESH,
            )
            x_copies[h, d].start()

    for s in range(len(OFFSETS)):
        lo = lax.rem(send_ref[s : s + 1, :], LO)
        hot_ref[s] = ones_where(lax.broadcasted_iota(I32, (LO, halo), 0) == lo)

    ids = hub_ref[...]
    hubs = ids.shape[1]
    owner = lax.div(ids, rows)
    local_row = lax.rem(ids, rows)
    owned = lax.broadcasted_iota(I32, (n_dom, hubs), 0) == owner
    before = ones_where(
        lax.broadcasted_iota(I32, (hubs, hubs), 0) < lax.broadcasted_iota(I32, (hubs, hubs), 1)
    )
    earlier = dot(ones_where(owned), before)
    rank = jnp.sum(jnp.where(owned, earlier, 0.0), 0, keepdims=True).astype(I32)
    place = lax.rem(rank + y * HUB_MOST, BLK)
    taken = ones_where(
        (lax.broadcasted_iota(I32, (BLK, hubs), 0) == place) & (owner == p)
    )
    halves = jnp.concatenate(
        [lax.rem(local_row, LO).astype(F32), (lax.div(local_row, LO) + 1).astype(F32)]
        + [jnp.zeros((14, hubs), F32)],
        0,
    ).astype(BF16)
    listed = dot(halves, taken, 1, 1)
    hub_lo = listed[0:1].astype(I32)
    hub_hi = listed[1:2].astype(I32) - 1
    hubhot_ref[...] = ones_where(lax.broadcasted_iota(I32, (LO, BLK), 0) == hub_lo)
    packed = Y_RING * HUB_MOST
    end_place = lax.rem(owner, Y_RING) * HUB_MOST + rank
    end_z = lax.div(owner, Y_RING)
    endhot_ref[...] = ones_where(lax.broadcasted_iota(I32, (packed, hubs), 0) == end_place)

    started = []
    hub_copies = {}
    for h in range(n_chunk):
        span = slice(h * chunk, (h + 1) * chunk)
        for d in range(1, n_feat):
            x_copies[h, d].wait()
        total = part_ref[j, span, :]
        for d in range(1, n_feat):
            total = total + rx[h, d - 1].astype(F32)
        proj = total.astype(BF16)
        for b in range(own_blocks):
            ext_ref[b, span, :] = proj[:, b * BLK : (b + 1) * BLK]
        stacked = jnp.concatenate([proj[:, g * LO : (g + 1) * LO] for g in range(his)], 0)

        mine = pick_groups(dot(stacked, hubhot_ref[...]), hub_hi, his, chunk).astype(BF16)
        hub_out[h] = mine
        hy[h, y] = mine
        for d in range(1, Y_RING):
            hub_copies[h, d] = pltpu.make_async_remote_copy(
                src_ref=hub_out.at[h],
                dst_ref=hy.at[h, y],
                send_sem=hys.at[h, d - 1],
                recv_sem=hyr.at[h, d - 1],
                device_id={"dom": y_at(d)},
                device_id_type=MESH,
            )
            hub_copies[h, d].start()

        for s in SEND_ORDER:
            target = p + OFFSETS[s]
            here = (target >= 0) & (target < n_dom)
            hi = jnp.where(here, lax.div(send_ref[s : s + 1, :], LO), -1)
            rows_out = pick_groups(dot(stacked, hot_ref[s]), hi, his, chunk).astype(BF16)
            for b in range(slot_blocks):
                sy[h, s, b] = rows_out[:, b * BLK : (b + 1) * BLK]
            first = own_blocks + s * slot_blocks
            copy = pltpu.make_async_remote_copy(
                src_ref=sy.at[h, s],
                dst_ref=ext_ref.at[first : first + slot_blocks, span, :],
                send_sem=sys_.at[h, s],
                recv_sem=syr.at[h, s],
                device_id={"dom": dom_at(OFFSETS[s])},
                device_id_type=MESH,
            )
            copy.start()
            started.append(copy)

    for h in range(n_chunk):
        for d in range(1, Y_RING):
            hub_copies[h, d].wait()
        for t in range(packed // BLK):
            lane = lax.broadcasted_iota(I32, (chunk, BLK), 1) + t * BLK
            tile = jnp.zeros((chunk, BLK), F32)
            for source in range(Y_RING):
                low, high = source * HUB_MOST, (source + 1) * HUB_MOST
                if high <= t * BLK or low >= (t + 1) * BLK:
                    continue
                tile = jnp.where((lane >= low) & (lane < high), hy[h, source].astype(F32), tile)
            hpack[h * chunk : (h + 1) * chunk, t * BLK : (t + 1) * BLK] = tile.astype(BF16)
    hz[z] = hpack[...]
    z_copies = []
    for d in range(1, z_ring):
        copy = pltpu.make_async_remote_copy(
            src_ref=hpack,
            dst_ref=hz.at[z],
            send_sem=hzs.at[d - 1],
            recv_sem=hzr.at[d - 1],
            device_id={"dom": z_at(d)},
            device_id_type=MESH,
        )
        copy.start()
        z_copies.append(copy)
    for copy in z_copies:
        copy.wait()
    everyone = jnp.concatenate([hz[source] for source in range(z_ring)], 0)
    hub_block = pick_groups(dot(everyone, endhot_ref[...]), end_z, z_ring, cols).astype(BF16)
    for b in range(hubs // BLK):
        ext_ref[hub_first + b] = hub_block[:, b * BLK : (b + 1) * BLK]

    for copy in started:
        copy.wait()


def tile_kernel(rows_ref, cols_ref, count_ref, tiles_ref, ext_ref, bias_ref, out_ref, acc_ref):
    live = count_ref[0]
    row_blocks = acc_ref.shape[0] - 1
    columns = acc_ref.shape[1]
    acc_ref[...] = jnp.zeros_like(acc_ref)
    unroll = 4

    @pl.loop(0, tiles_ref.shape[0] // unroll)
    def _(step):
        products = []
        for u in range(unroll):
            t = step * unroll + u
            products.append(dot(ext_ref[cols_ref[t]], tiles_ref[t], 1, 1))
        for u in range(unroll):
            t = step * unroll + u
            row = jnp.where(t < live, rows_ref[t], row_blocks)
            acc_ref[row] += products[u]

    eye = lax.broadcasted_iota(I32, (columns, columns), 0) == lax.broadcasted_iota(
        I32, (columns, columns), 1
    )
    bias = jnp.sum(jnp.where(eye, bias_ref[...], 0.0), 1, keepdims=True)
    for b in range(row_blocks):
        out_ref[:, b * BLK : (b + 1) * BLK] = jnp.maximum(acc_ref[b] + bias, 0.0).astype(BF16)


def local(
    n_dom, n_feat,
    features, weight, out_bias, tile_values, tile_rows, tile_cols, tile_count, send_rows, hub_ids,
):
    rows, _ = features.shape
    cols = out_bias.shape[0]
    hid = weight.shape[1]
    hubs = hub_ids.shape[0]
    slots, halo = send_rows.shape[1:]
    chunk = 16
    n_chunk = cols // chunk
    z_ring = n_dom // Y_RING
    blocks = (rows + slots * halo + hubs) // BLK
    vmem = pl.BlockSpec(memory_space=pltpu.VMEM)
    smem = pl.BlockSpec(memory_space=pltpu.SMEM)
    dma = pltpu.SemaphoreType.DMA
    extended = pl.pallas_call(
        functools.partial(exchange_kernel, n_dom, n_feat, cols, chunk),
        out_shape=jax.ShapeDtypeStruct((blocks, cols, BLK), BF16),
        in_specs=[vmem] * 4,
        out_specs=vmem,
        scratch_shapes=[
            pltpu.VMEM((n_feat, cols, rows), F32),
            pltpu.VMEM((slots, LO, halo), BF16),
            pltpu.VMEM((LO, BLK), BF16),
            pltpu.VMEM((Y_RING * HUB_MOST, hubs), BF16),
            pltpu.VMEM((n_feat, n_chunk, chunk, rows), BF16),
            pltpu.VMEM((n_chunk, n_feat - 1, chunk, rows), BF16),
            pltpu.VMEM((n_chunk, slots, halo // BLK, chunk, BLK), BF16),
            pltpu.VMEM((n_chunk, chunk, BLK), BF16),
            pltpu.VMEM((n_chunk, Y_RING, chunk, BLK), BF16),
            pltpu.VMEM((cols, Y_RING * HUB_MOST), BF16),
            pltpu.VMEM((z_ring, cols, Y_RING * HUB_MOST), BF16),
            dma((n_chunk, n_feat - 1)),
            dma((n_chunk, n_feat - 1)),
            dma((n_chunk, slots)),
            dma((n_chunk, slots)),
            dma((n_chunk, Y_RING - 1)),
            dma((n_chunk, Y_RING - 1)),
            dma((z_ring - 1,)),
            dma((z_ring - 1,)),
        ],
        compiler_params=pltpu.CompilerParams(
            collective_id=0, has_side_effects=True, vmem_limit_bytes=40 * 2**20
        ),
        name="exchange",
    )(features.T, weight, send_rows[0], hub_ids[None, :])
    out_t = pl.pallas_call(
        tile_kernel,
        out_shape=jax.ShapeDtypeStruct((cols, rows), BF16),
        in_specs=[smem, smem, smem, vmem, vmem, vmem],
        out_specs=vmem,
        scratch_shapes=[pltpu.VMEM((rows // BLK + 1, cols, BLK), F32)],
        name="tiles",
    )(tile_rows, tile_cols, tile_count, tile_values, extended, out_bias[None, :])
    return out_t.T


def solution(mesh):
    in_specs = (
        P("dom", "feat"),
        P(),
        P("feat"),
        P("dom", None, None),
        P("dom"),
        P("dom"),
        P("dom"),
        P("dom", None, None),
        P(),
    )
    out_specs = P("dom", "feat")
    body = functools.partial(local, mesh.shape["dom"], mesh.shape["feat"])
    return jax.shard_map(body, mesh=mesh, in_specs=in_specs, out_specs=out_specs, check_vma=False)
```

```python
import functools

import jax
import jax.numpy as jnp
from jax import lax
from jax.experimental import pallas as pl
from jax.experimental.pallas import tpu as pltpu
from jax.sharding import PartitionSpec as P

REACH = 4
HUB_MOST = 48
Y_RING = 8
LO = 256
BLK = 128
OFFSETS = tuple(range(-REACH, 0)) + tuple(range(1, REACH + 1))
SEND_ORDER = (0, 7, 1, 6, 2, 5, 3, 4)
VMEM_MOST = 67_043_328
MESH = pl.DeviceIdType.MESH
F32, BF16, I32 = jnp.float32, jnp.bfloat16, jnp.int32


def dims(a, b):
    return (((a,), (b,)), ((), ()))


def dot(a, b, ca=1, cb=0):
    return lax.dot_general(a, b, dims(ca, cb), preferred_element_type=F32)


def ones_where(mask):
    return jnp.where(mask, 1.0, 0.0).astype(BF16)


def pick_groups(stacked, group_of, groups, height):
    total = None
    for g in range(groups):
        part = jnp.where(group_of == g, stacked[g * height : (g + 1) * height], 0.0)
        total = part if total is None else total + part
    return total


def exchange_kernel(
    n_dom, n_feat, cols, chunk,
    ft_hbm, w_hbm, send_hbm, hub_hbm, tiles_hbm, rows_hbm, cols_hbm, count_hbm, bias_hbm,
    ext_ref, tiles_ref, meta_ref, bias_ref,
    ft_ref, w_ref, send_ref, hub_ref, hot_ref, endhot_ref, sx, rx, sy,
    hx_out, hx, hub_out, hy, hpack, hz, meta_in, count_in, bias_in,
    in_sem, sxs, sxr, sys_, syr, hxs, hxr, hys, hyr, hzs, hzr, feat_in, near_in, ring_in,
):
    p = lax.axis_index("dom")
    j = lax.axis_index("feat")
    y = lax.rem(p, Y_RING)
    z = lax.div(p, Y_RING)
    z_ring = n_dom // Y_RING
    k_in, rows = ft_ref.shape
    n_chunk = cols // chunk
    his = rows // LO
    slots, halo = send_ref.shape
    own_blocks = rows // BLK
    slot_blocks = halo // BLK
    hub_first = own_blocks + slots * slot_blocks
    near_desk, ring_desk = n_feat - 1, n_feat - 2

    loads = []
    for i, (src, dst) in enumerate(
        (
            (hub_hbm, hub_ref), (ft_hbm, ft_ref), (w_hbm, w_ref), (send_hbm, send_ref),
            (rows_hbm, meta_in.at[0]), (cols_hbm, meta_in.at[1]),
            (count_hbm, count_in), (bias_hbm, bias_in), (tiles_hbm, tiles_ref),
        )
    ):
        loads.append(pltpu.make_async_copy(src, dst, in_sem.at[i]))
        loads[-1].start()

    def y_at(step):
        return z * Y_RING + lax.rem(y + step, Y_RING)

    def z_at(step):
        return lax.rem(z + step, z_ring) * Y_RING + y

    def feat_at(step):
        return lax.rem(j + step, n_feat)

    def tell(sem, dom, feat):
        pl.semaphore_signal(
            sem, inc=1, device_id={"dom": dom, "feat": feat}, device_id_type=MESH
        )

    def inside(o):
        return (p + o >= 0) & (p + o < n_dom)

    barrier = pltpu.get_barrier_semaphore()
    for other in range(ring_desk):

        @pl.when(j != other)
        def _():
            tell(barrier, p, other)

    loads[0].wait()
    ids = hub_ref[...]
    hubs = ids.shape[1]
    owner = lax.div(ids, rows)
    local_row = lax.rem(ids, rows)
    owned = lax.broadcasted_iota(I32, (n_dom, hubs), 0) == owner
    before = ones_where(
        lax.broadcasted_iota(I32, (hubs, hubs), 0) < lax.broadcasted_iota(I32, (hubs, hubs), 1)
    )
    earlier = dot(ones_where(owned), before)
    rank = jnp.sum(jnp.where(owned, earlier, 0.0), 0, keepdims=True).astype(I32)
    place = lax.rem(rank + y * HUB_MOST, BLK)
    taken = ones_where((lax.broadcasted_iota(I32, (BLK, hubs), 0) == place) & (owner == p))
    halves = jnp.concatenate(
        [lax.rem(local_row, LO).astype(F32), (lax.div(local_row, LO) + 1).astype(F32)]
        + [jnp.zeros((14, hubs), F32)],
        0,
    ).astype(BF16)
    listed = dot(halves, taken, 1, 1)
    hub_row = (listed[0:1] + LO * (listed[1:2] - 1.0)).astype(I32)
    hub_pick = ones_where(lax.broadcasted_iota(I32, (rows, BLK), 0) == hub_row)

    f_in = w_ref.shape[0]
    loads[2].wait()
    pick = ones_where(
        lax.broadcasted_iota(I32, (BLK, f_in), 1)
        == lax.broadcasted_iota(I32, (BLK, f_in), 0) + j * k_in
    )
    w_mine = dot(pick, w_ref[...])
    w_t = w_mine.T.astype(BF16)[:, :k_in]

    loads[1].wait()
    ft = ft_ref[...]
    hub_ft = dot(ft, hub_pick).astype(BF16)
    hub_part = dot(w_t, hub_ft).astype(BF16)
    for d in range(n_feat):
        hx_out[d] = hub_part[d * cols : (d + 1) * cols]

    @pl.when(j < ring_desk)
    def _():
        pl.semaphore_wait(barrier, n_feat - 1)

    @pl.when(j == 0)
    def _():
        tell(feat_in, p, near_desk)
        tell(feat_in, p, ring_desk)

    @pl.when(j >= ring_desk)
    def _():
        pl.semaphore_wait(feat_in, 1)

    @pl.when(j == near_desk)
    def _():
        for o in OFFSETS:

            @pl.when(inside(o))
            def _():
                tell(barrier, p + o, near_desk)

        for d in range(1, Y_RING):
            tell(barrier, y_at(d), near_desk)

    @pl.when(j == ring_desk)
    def _():
        for d in range(1, z_ring):
            tell(barrier, z_at(d), ring_desk)

    hub_x = []
    for d in range(1, n_feat):
        copy = pltpu.make_async_remote_copy(
            src_ref=hx_out.at[feat_at(d)],
            dst_ref=hx.at[d - 1],
            send_sem=hxs.at[d - 1],
            recv_sem=hxr.at[d - 1],
            device_id={"feat": feat_at(d)},
            device_id_type=MESH,
        )
        copy.start()
        hub_x.append(copy)

    x_copies = {}
    for h in range(n_chunk):
        left = jnp.concatenate(
            [w_t[d * cols + h * chunk : d * cols + (h + 1) * chunk] for d in range(n_feat)], 0
        )
        part = dot(left, ft).astype(BF16)
        for d in range(n_feat):
            sx[d, h] = part[d * chunk : (d + 1) * chunk]
        for d in range(1, n_feat):
            x_copies[h, d] = pltpu.make_async_remote_copy(
                src_ref=sx.at[feat_at(d), h],
                dst_ref=rx.at[h, d - 1],
                send_sem=sxs.at[h, d - 1],
                recv_sem=sxr.at[h, d - 1],
                device_id={"feat": feat_at(d)},
                device_id_type=MESH,
            )
            x_copies[h, d].start()

    for copy in hub_x:
        copy.wait()
    hub_sum = hx_out[j].astype(F32)
    for d in range(1, n_feat):
        hub_sum = hub_sum + hx[d - 1].astype(F32)
    hub_mine = hub_sum.astype(BF16)
    hub_out[...] = hub_mine
    hy[y] = hub_mine

    @pl.when(j == near_desk)
    def _():
        before_p = lax.min(p, REACH)
        after_p = lax.min(n_dom - 1 - p, REACH)
        pl.semaphore_wait(barrier, before_p + after_p + Y_RING - 1)
        for other in range(n_feat - 1):
            tell(near_in, p, other)

    @pl.when(j != near_desk)
    def _():
        pl.semaphore_wait(near_in, 1)

    hub_y = []
    for d in range(1, Y_RING):
        copy = pltpu.make_async_remote_copy(
            src_ref=hub_out,
            dst_ref=hy.at[y],
            send_sem=hys.at[d - 1],
            recv_sem=hyr.at[d - 1],
            device_id={"dom": y_at(d)},
            device_id_type=MESH,
        )
        copy.start()
        hub_y.append(copy)

    loads[3].wait()
    for s in range(slots):
        lo = lax.rem(send_ref[s : s + 1, :], LO)
        hot_ref[s] = ones_where(lax.broadcasted_iota(I32, (LO, halo), 0) == lo)
    packed = Y_RING * HUB_MOST
    end_place = lax.rem(owner, Y_RING) * HUB_MOST + rank
    end_z = lax.div(owner, Y_RING)
    endhot_ref[...] = ones_where(lax.broadcasted_iota(I32, (packed, hubs), 0) == end_place)

    for i in range(4, 8):
        loads[i].wait()
    tiles = meta_in.shape[2]
    live = lax.broadcasted_iota(I32, (1, tiles), 1) < count_in[0]
    meta_ref[0:1, 0:tiles] = jnp.where(live, meta_in[0], own_blocks)
    meta_ref[1:2, 0:tiles] = meta_in[1]
    eye = lax.broadcasted_iota(I32, (cols, cols), 0) == lax.broadcasted_iota(I32, (cols, cols), 1)
    bias = jnp.sum(jnp.where(eye, bias_in[...], 0.0), 1, keepdims=True)
    bias_ref[...] = jnp.broadcast_to(bias, (cols, BLK))

    for s in range(slots):

        @pl.when(jnp.logical_not(inside(-OFFSETS[s])))
        def _():
            first = own_blocks + s * slot_blocks
            ext_ref[first : first + slot_blocks] = jnp.zeros((slot_blocks, cols, BLK), BF16)

    y_copies = {}

    def bulk(h):
        span = slice(h * chunk, (h + 1) * chunk)
        for d in range(1, n_feat):
            x_copies[h, d].wait()
        total = sx[j, h].astype(F32)
        for d in range(1, n_feat):
            total = total + rx[h, d - 1].astype(F32)
        proj = total.astype(BF16)
        for b in range(own_blocks):
            ext_ref[b, span, :] = proj[:, b * BLK : (b + 1) * BLK]
        stacked = jnp.concatenate([proj[:, g * LO : (g + 1) * LO] for g in range(his)], 0)
        for s in SEND_ORDER:
            hi = lax.div(send_ref[s : s + 1, :], LO)
            rows_out = pick_groups(dot(stacked, hot_ref[s]), hi, his, chunk).astype(BF16)
            for b in range(slot_blocks):
                sy[h, s, b] = rows_out[:, b * BLK : (b + 1) * BLK]
            first = own_blocks + s * slot_blocks
            y_copies[h, s] = pltpu.make_async_remote_copy(
                src_ref=sy.at[h, s],
                dst_ref=ext_ref.at[first : first + slot_blocks, span, :],
                send_sem=sys_.at[h, s],
                recv_sem=syr.at[h, s],
                device_id={"dom": p + OFFSETS[s]},
                device_id_type=MESH,
            )

            @pl.when(inside(OFFSETS[s]))
            def _():
                y_copies[h, s].start()

    bulk(0)

    for copy in hub_y:
        copy.wait()
    for t in range(packed // BLK):
        lane = lax.broadcasted_iota(I32, (cols, BLK), 1) + t * BLK
        tile = jnp.zeros((cols, BLK), F32)
        for source in range(Y_RING):
            low, high = source * HUB_MOST, (source + 1) * HUB_MOST
            if high <= t * BLK or low >= (t + 1) * BLK:
                continue
            tile = jnp.where((lane >= low) & (lane < high), hy[source].astype(F32), tile)
        hpack[:, t * BLK : (t + 1) * BLK] = tile.astype(BF16)
    hz[z] = hpack[...]

    @pl.when(j == ring_desk)
    def _():
        pl.semaphore_wait(barrier, z_ring - 1)
        for other in range(n_feat):
            if other != ring_desk:
                tell(ring_in, p, other)

    @pl.when(j != ring_desk)
    def _():
        pl.semaphore_wait(ring_in, 1)

    hub_z = []
    for d in range(1, z_ring):
        copy = pltpu.make_async_remote_copy(
            src_ref=hpack,
            dst_ref=hz.at[z],
            send_sem=hzs.at[d - 1],
            recv_sem=hzr.at[d - 1],
            device_id={"dom": z_at(d)},
            device_id_type=MESH,
        )
        copy.start()
        hub_z.append(copy)

    for h in range(1, n_chunk):
        bulk(h)

    for copy in hub_z:
        copy.wait()
    everyone = jnp.concatenate([hz[source] for source in range(z_ring)], 0)
    hub_block = pick_groups(dot(everyone, endhot_ref[...]), end_z, z_ring, cols).astype(BF16)
    for b in range(hubs // BLK):
        ext_ref[hub_first + b] = hub_block[:, b * BLK : (b + 1) * BLK]

    loads[8].wait()
    for (h, s), copy in y_copies.items():

        @pl.when(inside(OFFSETS[s]))
        def _():
            copy.wait_send()

        @pl.when(inside(-OFFSETS[s]))
        def _():
            copy.wait_recv()


def tile_kernel(meta_ref, tiles_ref, ext_ref, bias_ref, out_ref, acc_ref):
    row_blocks = acc_ref.shape[0] - 1
    acc_ref[...] = jnp.zeros_like(acc_ref)
    unroll = 6

    @pl.loop(0, tiles_ref.shape[0] // unroll)
    def _(step):
        products = []
        for u in range(unroll):
            t = step * unroll + u
            products.append(dot(ext_ref[meta_ref[1, t]], tiles_ref[t], 1, 1))
        for u in range(unroll):
            acc_ref[meta_ref[0, step * unroll + u]] += products[u]

    bias = bias_ref[...]
    for b in range(row_blocks):
        out_ref[:, b * BLK : (b + 1) * BLK] = jnp.maximum(acc_ref[b] + bias, 0.0).astype(BF16)


def local(
    n_dom, n_feat,
    features, weight, out_bias, tile_values, tile_rows, tile_cols, tile_count, send_rows, hub_ids,
):
    rows, _ = features.shape
    cols = out_bias.shape[0]
    hubs = hub_ids.shape[0]
    slots, halo = send_rows.shape[1:]
    chunk = 16
    n_chunk = cols // chunk
    z_ring = n_dom // Y_RING
    blocks = (rows + slots * halo + hubs) // BLK
    vmem = pl.BlockSpec(memory_space=pltpu.VMEM)
    dma = pltpu.SemaphoreType.DMA
    tiles = tile_values.shape[0]
    shape = jax.ShapeDtypeStruct
    carried = 2 * blocks * cols * BLK + 2 * tile_values.size + 4 * (8 + cols) * BLK
    extended, held_tiles, meta, bias = pl.pallas_call(
        functools.partial(exchange_kernel, n_dom, n_feat, cols, chunk),
        out_shape=(
            pltpu.VMEM((blocks, cols, BLK), BF16),
            pltpu.VMEM(tile_values.shape, BF16),
            pltpu.VMEM((8, BLK), I32),
            pltpu.VMEM((cols, BLK), F32),
        ),
        in_specs=[pl.BlockSpec(memory_space=pltpu.HBM)] * 9,
        out_specs=(vmem,) * 4,
        scratch_shapes=[
            pltpu.VMEM((features.shape[1], rows), BF16),
            pltpu.VMEM(weight.shape, BF16),
            pltpu.VMEM((slots, halo), I32),
            pltpu.VMEM((1, hubs), I32),
            pltpu.VMEM((slots, LO, halo), BF16),
            pltpu.VMEM((Y_RING * HUB_MOST, hubs), BF16),
            pltpu.VMEM((n_feat, n_chunk, chunk, rows), BF16),
            pltpu.VMEM((n_chunk, n_feat - 1, chunk, rows), BF16),
            pltpu.VMEM((n_chunk, slots, halo // BLK, chunk, BLK), BF16),
            pltpu.VMEM((n_feat, cols, BLK), BF16),
            pltpu.VMEM((n_feat - 1, cols, BLK), BF16),
            pltpu.VMEM((cols, BLK), BF16),
            pltpu.VMEM((Y_RING, cols, BLK), BF16),
            pltpu.VMEM((cols, Y_RING * HUB_MOST), BF16),
            pltpu.VMEM((z_ring, cols, Y_RING * HUB_MOST), BF16),
            pltpu.VMEM((2, 1, tiles), I32),
            pltpu.SMEM((1,), I32),
            pltpu.VMEM((1, cols), F32),
            dma((9,)),
            dma((n_chunk, n_feat - 1)),
            dma((n_chunk, n_feat - 1)),
            dma((n_chunk, slots)),
            dma((n_chunk, slots)),
            dma((n_feat - 1,)),
            dma((n_feat - 1,)),
            dma((Y_RING - 1,)),
            dma((Y_RING - 1,)),
            dma((z_ring - 1,)),
            dma((z_ring - 1,)),
            pltpu.SemaphoreType.REGULAR,
            pltpu.SemaphoreType.REGULAR,
            pltpu.SemaphoreType.REGULAR,
        ],
        compiler_params=pltpu.CompilerParams(
            collective_id=0,
            has_side_effects=True,
            vmem_limit_bytes=VMEM_MOST - carried - 65536,
        ),
        name="exchange",
    )(
        features.T, weight, send_rows[0], hub_ids[None, :], tile_values,
        tile_rows[None, :], tile_cols[None, :], tile_count, out_bias[None, :],
    )
    out_t = pl.pallas_call(
        tile_kernel,
        out_shape=shape((cols, rows), BF16),
        in_specs=[pl.BlockSpec(memory_space=pltpu.SMEM), vmem, vmem, vmem],
        out_specs=vmem,
        scratch_shapes=[pltpu.VMEM((rows // BLK + 1, cols, BLK), F32)],
        compiler_params=pltpu.CompilerParams(vmem_limit_bytes=16 * 2**20),
        name="tiles",
    )(meta, held_tiles, extended, bias)
    return out_t.T


def solution(mesh):
    in_specs = (
        P("dom", "feat"),
        P(),
        P("feat"),
        P("dom", None, None),
        P("dom"),
        P("dom"),
        P("dom"),
        P("dom", None, None),
        P(),
    )
    out_specs = P("dom", "feat")
    body = functools.partial(local, mesh.shape["dom"], mesh.shape["feat"])
    return jax.shard_map(body, mesh=mesh, in_specs=in_specs, out_specs=out_specs, check_vma=False)
```

```python
import functools

import jax
import jax.numpy as jnp
from jax import lax
from jax.experimental import pallas as pl
from jax.experimental.pallas import tpu as pltpu
from jax.sharding import PartitionSpec as P

REACH = 4
HUB_MOST = 48
Y_RING = 8
LO = 256
BLK = 128
OFFSETS = tuple(range(-REACH, 0)) + tuple(range(1, REACH + 1))
SEND_ORDER = (0, 7, 1, 6, 2, 5, 3, 4)
VMEM_MOST = 67_043_328
MESH = pl.DeviceIdType.MESH
F32, BF16, I32 = jnp.float32, jnp.bfloat16, jnp.int32


def dims(a, b):
    return (((a,), (b,)), ((), ()))


def dot(a, b, ca=1, cb=0):
    return lax.dot_general(a, b, dims(ca, cb), preferred_element_type=F32)


def ones_where(mask):
    return jnp.where(mask, 1.0, 0.0).astype(BF16)


def pick_groups(stacked, group_of, groups, height):
    total = None
    for g in range(groups):
        part = jnp.where(group_of == g, stacked[g * height : (g + 1) * height], 0.0)
        total = part if total is None else total + part
    return total


def exchange_kernel(
    n_dom, n_feat, cols, chunk,
    ft_hbm, w_hbm, send_hbm, hub_hbm, tiles_hbm, rows_hbm, cols_hbm, count_hbm, bias_hbm,
    ext_ref, tiles_ref, meta_ref, bias_ref,
    ft_ref, w_ref, send_ref, hub_ref, hot_ref, endhot_ref, sx, rx, sy,
    hx_out, hx, hub_out, hy, hpack, hz, meta_in, count_in, bias_in,
    in_sem, sxs, sxr, sys_, syr, hxs, hxr, hys, hyr, hzs, hzr, feat_in, near_in, ring_in,
):
    p = lax.axis_index("dom")
    j = lax.axis_index("feat")
    y = lax.rem(p, Y_RING)
    z = lax.div(p, Y_RING)
    z_ring = n_dom // Y_RING
    k_in, rows = ft_ref.shape
    n_chunk = cols // chunk
    his = rows // LO
    slots, halo = send_ref.shape
    own_blocks = rows // BLK
    slot_blocks = halo // BLK
    hub_first = own_blocks + slots * slot_blocks
    near_desk, ring_desk = n_feat - 1, n_feat - 2

    loads = []
    for i, (src, dst) in enumerate(
        (
            (hub_hbm, hub_ref), (ft_hbm, ft_ref), (w_hbm, w_ref), (send_hbm, send_ref),
            (rows_hbm, meta_in.at[0]), (cols_hbm, meta_in.at[1]),
            (count_hbm, count_in), (bias_hbm, bias_in), (tiles_hbm, tiles_ref),
        )
    ):
        loads.append(pltpu.make_async_copy(src, dst, in_sem.at[i]))
        loads[-1].start()

    def y_at(step):
        return z * Y_RING + lax.rem(y + step, Y_RING)

    def z_at(step):
        return lax.rem(z + step, z_ring) * Y_RING + y

    def feat_at(step):
        return lax.rem(j + step, n_feat)

    def tell(sem, dom, feat):
        pl.semaphore_signal(
            sem, inc=1, device_id={"dom": dom, "feat": feat}, device_id_type=MESH
        )

    def inside(o):
        return (p + o >= 0) & (p + o < n_dom)

    barrier = pltpu.get_barrier_semaphore()
    for other in range(ring_desk):

        @pl.when(j != other)
        def _():
            tell(barrier, p, other)

    loads[0].wait()
    ids = hub_ref[...]
    hubs = ids.shape[1]
    owner = lax.div(ids, rows)
    local_row = lax.rem(ids, rows)
    owned = lax.broadcasted_iota(I32, (n_dom, hubs), 0) == owner
    before = ones_where(
        lax.broadcasted_iota(I32, (hubs, hubs), 0) < lax.broadcasted_iota(I32, (hubs, hubs), 1)
    )
    earlier = dot(ones_where(owned), before)
    rank = jnp.sum(jnp.where(owned, earlier, 0.0), 0, keepdims=True).astype(I32)
    place = lax.rem(rank + y * HUB_MOST, BLK)
    taken = ones_where((lax.broadcasted_iota(I32, (BLK, hubs), 0) == place) & (owner == p))
    halves = jnp.concatenate(
        [lax.rem(local_row, LO).astype(F32), (lax.div(local_row, LO) + 1).astype(F32)]
        + [jnp.zeros((14, hubs), F32)],
        0,
    ).astype(BF16)
    listed = dot(halves, taken, 1, 1)
    hub_row = (listed[0:1] + LO * (listed[1:2] - 1.0)).astype(I32)
    hub_pick = ones_where(lax.broadcasted_iota(I32, (rows, BLK), 0) == hub_row)

    f_in = w_ref.shape[0]
    loads[2].wait()
    pick = ones_where(
        lax.broadcasted_iota(I32, (BLK, f_in), 1)
        == lax.broadcasted_iota(I32, (BLK, f_in), 0) + j * k_in
    )
    w_mine = dot(pick, w_ref[...])
    w_t = w_mine.T.astype(BF16)[:, :k_in]

    loads[1].wait()
    ft = ft_ref[...]
    hub_ft = dot(ft, hub_pick).astype(BF16)
    hub_part = dot(w_t, hub_ft).astype(BF16)
    for d in range(n_feat):
        hx_out[d] = hub_part[d * cols : (d + 1) * cols]

    @pl.when(j < ring_desk)
    def _():
        pl.semaphore_wait(barrier, n_feat - 1)

    @pl.when(j == 0)
    def _():
        tell(feat_in, p, near_desk)
        tell(feat_in, p, ring_desk)

    @pl.when(j >= ring_desk)
    def _():
        pl.semaphore_wait(feat_in, 1)

    @pl.when(j == near_desk)
    def _():
        for o in OFFSETS:

            @pl.when(inside(o))
            def _():
                tell(barrier, p + o, near_desk)

        for d in range(1, Y_RING):
            tell(barrier, y_at(d), near_desk)

    @pl.when(j == ring_desk)
    def _():
        for d in range(1, z_ring):
            tell(barrier, z_at(d), ring_desk)

    hub_x = []
    for d in range(1, n_feat):
        copy = pltpu.make_async_remote_copy(
            src_ref=hx_out.at[feat_at(d)],
            dst_ref=hx.at[d - 1],
            send_sem=hxs.at[d - 1],
            recv_sem=hxr.at[d - 1],
            device_id={"feat": feat_at(d)},
            device_id_type=MESH,
        )
        copy.start()
        hub_x.append(copy)

    x_copies = {}
    for h in range(n_chunk):
        left = jnp.concatenate(
            [w_t[d * cols + h * chunk : d * cols + (h + 1) * chunk] for d in range(n_feat)], 0
        )
        part = dot(left, ft).astype(BF16)
        for d in range(n_feat):
            sx[d, h] = part[d * chunk : (d + 1) * chunk]
        for d in range(1, n_feat):
            x_copies[h, d] = pltpu.make_async_remote_copy(
                src_ref=sx.at[feat_at(d), h],
                dst_ref=rx.at[h, d - 1],
                send_sem=sxs.at[h, d - 1],
                recv_sem=sxr.at[h, d - 1],
                device_id={"feat": feat_at(d)},
                device_id_type=MESH,
            )
            x_copies[h, d].start()

    for copy in hub_x:
        copy.wait()
    hub_sum = hx_out[j].astype(F32)
    for d in range(1, n_feat):
        hub_sum = hub_sum + hx[d - 1].astype(F32)
    hub_mine = hub_sum.astype(BF16)
    hub_out[...] = hub_mine
    hy[y] = hub_mine

    @pl.when(j == near_desk)
    def _():
        before_p = lax.min(p, REACH)
        after_p = lax.min(n_dom - 1 - p, REACH)
        pl.semaphore_wait(barrier, before_p + after_p + Y_RING - 1)
        for other in range(n_feat - 1):
            tell(near_in, p, other)

    @pl.when(j != near_desk)
    def _():
        pl.semaphore_wait(near_in, 1)

    hub_y = []
    for d in range(1, Y_RING):
        copy = pltpu.make_async_remote_copy(
            src_ref=hub_out,
            dst_ref=hy.at[y],
            send_sem=hys.at[d - 1],
            recv_sem=hyr.at[d - 1],
            device_id={"dom": y_at(d)},
            device_id_type=MESH,
        )
        copy.start()
        hub_y.append(copy)

    loads[3].wait()
    for s in range(slots):
        lo = lax.rem(send_ref[s : s + 1, :], LO)
        hot_ref[s] = ones_where(lax.broadcasted_iota(I32, (LO, halo), 0) == lo)
    packed = Y_RING * HUB_MOST
    end_place = lax.rem(owner, Y_RING) * HUB_MOST + rank
    end_z = lax.div(owner, Y_RING)
    endhot_ref[...] = ones_where(lax.broadcasted_iota(I32, (packed, hubs), 0) == end_place)

    for i in range(4, 8):
        loads[i].wait()
    tiles = meta_in.shape[2]
    live = lax.broadcasted_iota(I32, (1, tiles), 1) < count_in[0]
    meta_ref[0:1, 0:tiles] = jnp.where(live, meta_in[0], own_blocks)
    meta_ref[1:2, 0:tiles] = meta_in[1]
    eye = lax.broadcasted_iota(I32, (cols, cols), 0) == lax.broadcasted_iota(I32, (cols, cols), 1)
    bias = jnp.sum(jnp.where(eye, bias_in[...], 0.0), 1, keepdims=True)
    bias_ref[...] = jnp.broadcast_to(bias, (cols, BLK))

    for s in range(slots):

        @pl.when(jnp.logical_not(inside(-OFFSETS[s])))
        def _():
            first = own_blocks + s * slot_blocks
            ext_ref[first : first + slot_blocks] = jnp.zeros((slot_blocks, cols, BLK), BF16)

    y_copies = {}

    def bulk(h):
        span = slice(h * chunk, (h + 1) * chunk)
        for d in range(1, n_feat):
            x_copies[h, d].wait()
        total = sx[j, h].astype(F32)
        for d in range(1, n_feat):
            total = total + rx[h, d - 1].astype(F32)
        proj = total.astype(BF16)
        for b in range(own_blocks):
            ext_ref[b, span, :] = proj[:, b * BLK : (b + 1) * BLK]
        stacked = jnp.concatenate([proj[:, g * LO : (g + 1) * LO] for g in range(his)], 0)
        for s in SEND_ORDER:
            hi = lax.div(send_ref[s : s + 1, :], LO)
            rows_out = pick_groups(dot(stacked, hot_ref[s]), hi, his, chunk).astype(BF16)
            for b in range(slot_blocks):
                sy[h, s, b] = rows_out[:, b * BLK : (b + 1) * BLK]
            first = own_blocks + s * slot_blocks
            y_copies[h, s] = pltpu.make_async_remote_copy(
                src_ref=sy.at[h, s],
                dst_ref=ext_ref.at[first : first + slot_blocks, span, :],
                send_sem=sys_.at[h, s],
                recv_sem=syr.at[h, s],
                device_id={"dom": p + OFFSETS[s]},
                device_id_type=MESH,
            )

            @pl.when(inside(OFFSETS[s]))
            def _():
                y_copies[h, s].start()

    bulk(0)
    bulk(1)

    for copy in hub_y:
        copy.wait()
    for t in range(packed // BLK):
        lane = lax.broadcasted_iota(I32, (cols, BLK), 1) + t * BLK
        tile = jnp.zeros((cols, BLK), F32)
        for source in range(Y_RING):
            low, high = source * HUB_MOST, (source + 1) * HUB_MOST
            if high <= t * BLK or low >= (t + 1) * BLK:
                continue
            tile = jnp.where((lane >= low) & (lane < high), hy[source].astype(F32), tile)
        hpack[:, t * BLK : (t + 1) * BLK] = tile.astype(BF16)
    hz[z] = hpack[...]

    @pl.when(j == ring_desk)
    def _():
        pl.semaphore_wait(barrier, z_ring - 1)
        for other in range(n_feat):
            if other != ring_desk:
                tell(ring_in, p, other)

    @pl.when(j != ring_desk)
    def _():
        pl.semaphore_wait(ring_in, 1)

    hub_z = []
    for d in range(1, z_ring):
        copy = pltpu.make_async_remote_copy(
            src_ref=hpack,
            dst_ref=hz.at[z],
            send_sem=hzs.at[d - 1],
            recv_sem=hzr.at[d - 1],
            device_id={"dom": z_at(d)},
            device_id_type=MESH,
        )
        copy.start()
        hub_z.append(copy)

    for h in range(2, n_chunk):
        bulk(h)

    for copy in hub_z:
        copy.wait()
    everyone = jnp.concatenate([hz[source] for source in range(z_ring)], 0)
    hub_block = pick_groups(dot(everyone, endhot_ref[...]), end_z, z_ring, cols).astype(BF16)
    for b in range(hubs // BLK):
        ext_ref[hub_first + b] = hub_block[:, b * BLK : (b + 1) * BLK]

    loads[8].wait()
    for (h, s), copy in y_copies.items():

        @pl.when(inside(OFFSETS[s]))
        def _():
            copy.wait_send()

        @pl.when(inside(-OFFSETS[s]))
        def _():
            copy.wait_recv()


def tile_kernel(meta_ref, tiles_ref, ext_ref, bias_ref, out_ref, acc_ref):
    row_blocks = acc_ref.shape[0] - 1
    acc_ref[...] = jnp.zeros_like(acc_ref)
    unroll = 36
    columns = ext_ref.shape[1]

    @pl.loop(0, tiles_ref.shape[0] // unroll)
    def _(step):
        products = []
        for u in range(0, unroll, 2):
            t = step * unroll + u
            left = jnp.concatenate([ext_ref[meta_ref[1, t]], ext_ref[meta_ref[1, t + 1]]], 0)
            both = dot(left, tiles_ref[pl.ds(t, 2)].reshape(2 * BLK, BLK), 1, 1)
            products += [both[:columns, :BLK], both[columns:, BLK:]]
        for u in range(unroll):
            acc_ref[meta_ref[0, step * unroll + u]] += products[u]

    bias = bias_ref[...]
    for b in range(row_blocks):
        out_ref[:, b * BLK : (b + 1) * BLK] = jnp.maximum(acc_ref[b] + bias, 0.0).astype(BF16)


def local(
    n_dom, n_feat,
    features, weight, out_bias, tile_values, tile_rows, tile_cols, tile_count, send_rows, hub_ids,
):
    rows, _ = features.shape
    cols = out_bias.shape[0]
    hubs = hub_ids.shape[0]
    slots, halo = send_rows.shape[1:]
    chunk = 8
    n_chunk = cols // chunk
    z_ring = n_dom // Y_RING
    blocks = (rows + slots * halo + hubs) // BLK
    vmem = pl.BlockSpec(memory_space=pltpu.VMEM)
    dma = pltpu.SemaphoreType.DMA
    tiles = tile_values.shape[0]
    shape = jax.ShapeDtypeStruct
    carried = 2 * blocks * cols * BLK + 2 * tile_values.size + 4 * (8 + cols) * BLK
    extended, held_tiles, meta, bias = pl.pallas_call(
        functools.partial(exchange_kernel, n_dom, n_feat, cols, chunk),
        out_shape=(
            pltpu.VMEM((blocks, cols, BLK), BF16),
            pltpu.VMEM(tile_values.shape, BF16),
            pltpu.VMEM((8, BLK), I32),
            pltpu.VMEM((cols, BLK), F32),
        ),
        in_specs=[pl.BlockSpec(memory_space=pltpu.HBM)] * 9,
        out_specs=(vmem,) * 4,
        scratch_shapes=[
            pltpu.VMEM((features.shape[1], rows), BF16),
            pltpu.VMEM(weight.shape, BF16),
            pltpu.VMEM((slots, halo), I32),
            pltpu.VMEM((1, hubs), I32),
            pltpu.VMEM((slots, LO, halo), BF16),
            pltpu.VMEM((Y_RING * HUB_MOST, hubs), BF16),
            pltpu.VMEM((n_feat, n_chunk, chunk, rows), BF16),
            pltpu.VMEM((n_chunk, n_feat - 1, chunk, rows), BF16),
            pltpu.VMEM((n_chunk, slots, halo // BLK, chunk, BLK), BF16),
            pltpu.VMEM((n_feat, cols, BLK), BF16),
            pltpu.VMEM((n_feat - 1, cols, BLK), BF16),
            pltpu.VMEM((cols, BLK), BF16),
            pltpu.VMEM((Y_RING, cols, BLK), BF16),
            pltpu.VMEM((cols, Y_RING * HUB_MOST), BF16),
            pltpu.VMEM((z_ring, cols, Y_RING * HUB_MOST), BF16),
            pltpu.VMEM((2, 1, tiles), I32),
            pltpu.SMEM((1,), I32),
            pltpu.VMEM((1, cols), F32),
            dma((9,)),
            dma((n_chunk, n_feat - 1)),
            dma((n_chunk, n_feat - 1)),
            dma((n_chunk, slots)),
            dma((n_chunk, slots)),
            dma((n_feat - 1,)),
            dma((n_feat - 1,)),
            dma((Y_RING - 1,)),
            dma((Y_RING - 1,)),
            dma((z_ring - 1,)),
            dma((z_ring - 1,)),
            pltpu.SemaphoreType.REGULAR,
            pltpu.SemaphoreType.REGULAR,
            pltpu.SemaphoreType.REGULAR,
        ],
        compiler_params=pltpu.CompilerParams(
            collective_id=0,
            has_side_effects=True,
            vmem_limit_bytes=VMEM_MOST - carried - 65536,
        ),
        name="exchange",
    )(
        features.T, weight, send_rows[0], hub_ids[None, :], tile_values,
        tile_rows[None, :], tile_cols[None, :], tile_count, out_bias[None, :],
    )
    out_t = pl.pallas_call(
        tile_kernel,
        out_shape=shape((cols, rows), BF16),
        in_specs=[pl.BlockSpec(memory_space=pltpu.SMEM), vmem, vmem, vmem],
        out_specs=vmem,
        scratch_shapes=[pltpu.VMEM((rows // BLK + 1, cols, BLK), F32)],
        compiler_params=pltpu.CompilerParams(vmem_limit_bytes=16 * 2**20),
        name="tiles",
    )(meta, held_tiles, extended, bias)
    return out_t.T


def solution(mesh):
    in_specs = (
        P("dom", "feat"),
        P(),
        P("feat"),
        P("dom", None, None),
        P("dom"),
        P("dom"),
        P("dom"),
        P("dom", None, None),
        P(),
    )
    out_specs = P("dom", "feat")
    body = functools.partial(local, mesh.shape["dom"], mesh.shape["feat"])
    return jax.shard_map(body, mesh=mesh, in_specs=in_specs, out_specs=out_specs, check_vma=False)
```

```python
import functools

import jax
import jax.numpy as jnp
from jax import lax
from jax.experimental import pallas as pl
from jax.experimental.pallas import tpu as pltpu
from jax.sharding import PartitionSpec as P

REACH = 4
HUB_MOST = 48
Y_RING = 8
LO = 256
BLK = 128
OFFSETS = tuple(range(-REACH, 0)) + tuple(range(1, REACH + 1))
SEND_ORDER = (0, 7, 1, 6, 2, 5, 3, 4)
VMEM_MOST = 67_043_328
MESH = pl.DeviceIdType.MESH
F32, BF16, I32 = jnp.float32, jnp.bfloat16, jnp.int32


def dims(a, b):
    return (((a,), (b,)), ((), ()))


def dot(a, b, ca=1, cb=0):
    return lax.dot_general(a, b, dims(ca, cb), preferred_element_type=F32)


def ones_where(mask):
    return jnp.where(mask, 1.0, 0.0).astype(BF16)


def ascending(shape, swap=False):
    a, b = lax.broadcasted_iota(I32, shape, 0), lax.broadcasted_iota(I32, shape, 1)
    return b < a if swap else a < b


def pick_groups(stacked, group_of, groups, height):
    total = jnp.zeros((height, stacked.shape[1]), F32)
    for g in range(groups):
        total = jnp.where(group_of == g, stacked[g * height : (g + 1) * height], total)
    return total


def as_row(x):
    return jnp.concatenate([x[i : i + 1] for i in range(x.shape[0])], 1)


def exchange_kernel(
    n_dom, n_feat, cols, chunk,
    ft_hbm, w_hbm, send_hbm, hub_hbm, tiles_hbm, rows_hbm, cols_hbm, count_hbm, bias_hbm,
    ext_ref, tiles_ref, meta_ref, bias_ref,
    ft_ref, w_ref, send_ref, hub_ref, hot_ref, endhot_ref, sx, rx, sy,
    hx_out, hx, hub_out, hy, hpack, hz, meta_in, count_in, bias_in,
    in_sem, sxs, sxr, sys_, syr, hxs, hxr, hys, hyr, hzs, hzr, feat_in, near_in, ring_in,
):
    p = lax.axis_index("dom")
    j = lax.axis_index("feat")
    y = lax.rem(p, Y_RING)
    z = lax.div(p, Y_RING)
    z_ring = n_dom // Y_RING
    k_in, rows = ft_ref.shape
    n_chunk = cols // chunk
    his = rows // LO
    slots, halo = send_ref.shape
    own_blocks = rows // BLK
    slot_blocks = halo // BLK
    hub_first = own_blocks + slots * slot_blocks
    near_desk, ring_desk = n_feat - 1, n_feat - 2

    loads = []
    for i, (src, dst) in enumerate(
        (
            (hub_hbm, hub_ref), (ft_hbm, ft_ref), (w_hbm, w_ref), (send_hbm, send_ref),
            (rows_hbm, meta_in.at[0]), (cols_hbm, meta_in.at[1]),
            (count_hbm, count_in), (bias_hbm, bias_in), (tiles_hbm, tiles_ref),
        )
    ):
        loads.append(pltpu.make_async_copy(src, dst, in_sem.at[i]))
        loads[-1].start()

    def y_at(step):
        return z * Y_RING + lax.rem(y + step, Y_RING)

    def z_at(step):
        return lax.rem(z + step, z_ring) * Y_RING + y

    def feat_at(step):
        return lax.rem(j + step, n_feat)

    def tell(sem, dom, feat):
        pl.semaphore_signal(
            sem, inc=1, device_id={"dom": dom, "feat": feat}, device_id_type=MESH
        )

    def inside(o):
        return (p + o >= 0) & (p + o < n_dom)

    barrier = pltpu.get_barrier_semaphore()
    for other in range(ring_desk):

        @pl.when(j != other)
        def _():
            tell(barrier, p, other)

    for i in range(3):
        loads[i].wait()

    ids = hub_ref[...]
    hubs = ids.size
    f_in = w_ref.shape[0]
    mine = lax.div(ids, rows) == p
    mine_ones = ones_where(mine)
    side = ids.shape[0]
    in_row = dot(mine_ones, ones_where(ascending((BLK, BLK))))
    above = jnp.sum(dot(ones_where(ascending((side, side), True)), mine_ones), 1, keepdims=True)
    my_rank = (in_row + above).astype(I32)
    local_row = lax.rem(ids, rows)
    place = as_row(jnp.where(mine, lax.rem(my_rank + y * HUB_MOST, BLK), -1))
    taken = ones_where(lax.broadcasted_iota(I32, (BLK, hubs), 0) == place)
    halves = jnp.concatenate(
        [as_row(lax.rem(local_row, LO).astype(F32)), as_row((lax.div(local_row, LO) + 1).astype(F32))]
        + [jnp.zeros((14, hubs), F32)],
        0,
    ).astype(BF16)
    listed = dot(halves, taken, 1, 1)
    hub_row = (listed[0:1] + LO * (listed[1:2] - 1.0)).astype(I32)
    hub_pick = ones_where(lax.broadcasted_iota(I32, (rows, BLK), 0) == hub_row)

    pick = ones_where(
        lax.broadcasted_iota(I32, (BLK, f_in), 1)
        == lax.broadcasted_iota(I32, (BLK, f_in), 0) + j * k_in
    )
    w_mine = dot(pick, w_ref[...])
    w_t = w_mine.T.astype(BF16)[:, :k_in]

    ft = ft_ref[...]
    hub_ft = dot(ft, hub_pick).astype(BF16)
    hub_part = dot(w_t, hub_ft)
    half = cols // 2
    for d in range(n_feat):
        lower = hub_part[d * cols : d * cols + half]
        upper = hub_part[d * cols + half : (d + 1) * cols]
        hx_out[d] = (lower + pltpu.roll(upper, BLK // 2, 1)).astype(BF16)

    @pl.when(j < ring_desk)
    def _():
        pl.semaphore_wait(barrier, n_feat - 1)

    @pl.when(j == 0)
    def _():
        tell(feat_in, p, near_desk)
        tell(feat_in, p, ring_desk)

    @pl.when(j >= ring_desk)
    def _():
        pl.semaphore_wait(feat_in, 1)

    @pl.when(j == near_desk)
    def _():
        for o in OFFSETS:

            @pl.when(inside(o))
            def _():
                tell(barrier, p + o, near_desk)

        for d in range(1, Y_RING):
            tell(barrier, y_at(d), near_desk)

    @pl.when(j == ring_desk)
    def _():
        for d in range(1, z_ring):
            tell(barrier, z_at(d), ring_desk)

    hub_x = []
    for d in range(1, n_feat):
        copy = pltpu.make_async_remote_copy(
            src_ref=hx_out.at[feat_at(d)],
            dst_ref=hx.at[d - 1],
            send_sem=hxs.at[d - 1],
            recv_sem=hxr.at[d - 1],
            device_id={"feat": feat_at(d)},
            device_id_type=MESH,
        )
        copy.start()
        hub_x.append(copy)

    x_copies = {}
    for h in range(n_chunk):
        left = jnp.concatenate(
            [w_t[d * cols + h * chunk : d * cols + (h + 1) * chunk] for d in range(n_feat)], 0
        )
        part = dot(left, ft).astype(BF16)
        for d in range(n_feat):
            sx[d, h] = part[d * chunk : (d + 1) * chunk]
        for d in range(1, n_feat):
            x_copies[h, d] = pltpu.make_async_remote_copy(
                src_ref=sx.at[feat_at(d), h],
                dst_ref=rx.at[h, d - 1],
                send_sem=sxs.at[h, d - 1],
                recv_sem=sxr.at[h, d - 1],
                device_id={"feat": feat_at(d)},
                device_id_type=MESH,
            )
            x_copies[h, d].start()

    loads[3].wait()
    for s in range(slots):
        lo = lax.rem(send_ref[s : s + 1, :], LO)
        hot_ref[s] = ones_where(lax.broadcasted_iota(I32, (LO, halo), 0) == lo)
    packed = Y_RING * HUB_MOST
    ids_row = as_row(ids)
    owner = lax.div(ids_row, rows)
    owned = lax.broadcasted_iota(I32, (n_dom, hubs), 0) == owner
    earlier = dot(ones_where(owned), ones_where(ascending((hubs, hubs))))
    rank = jnp.sum(jnp.where(owned, earlier, 0.0), 0, keepdims=True).astype(I32)
    end_place = lax.rem(owner, Y_RING) * HUB_MOST + rank
    end_z = lax.div(owner, Y_RING)
    endhot_ref[...] = ones_where(lax.broadcasted_iota(I32, (packed, hubs), 0) == end_place)

    for i in range(4, 8):
        loads[i].wait()
    tiles = meta_in.shape[2]
    live = lax.broadcasted_iota(I32, (1, tiles), 1) < count_in[0]
    meta_ref[0:1, 0:tiles] = jnp.where(live, meta_in[0], own_blocks)
    meta_ref[1:2, 0:tiles] = meta_in[1]
    eye = lax.broadcasted_iota(I32, (cols, cols), 0) == lax.broadcasted_iota(I32, (cols, cols), 1)
    bias = jnp.sum(jnp.where(eye, bias_in[...], 0.0), 1, keepdims=True)
    bias_ref[...] = jnp.broadcast_to(bias, (cols, BLK))

    for s in range(slots):

        @pl.when(jnp.logical_not(inside(-OFFSETS[s])))
        def _():
            first = own_blocks + s * slot_blocks
            ext_ref[first : first + slot_blocks] = jnp.zeros((slot_blocks, cols, BLK), BF16)

    for copy in hub_x:
        copy.wait()
    hub_sum = hx_out[j].astype(F32)
    for d in range(1, n_feat):
        hub_sum = hub_sum + hx[d - 1].astype(F32)
    hub_mine = hub_sum.astype(BF16)
    hub_out[...] = hub_mine
    hy[y] = hub_mine

    @pl.when(j == near_desk)
    def _():
        before_p = lax.min(p, REACH)
        after_p = lax.min(n_dom - 1 - p, REACH)
        pl.semaphore_wait(barrier, before_p + after_p + Y_RING - 1)
        for other in range(n_feat - 1):
            tell(near_in, p, other)

    @pl.when(j != near_desk)
    def _():
        pl.semaphore_wait(near_in, 1)

    hub_y = []
    for d in range(1, Y_RING):
        copy = pltpu.make_async_remote_copy(
            src_ref=hub_out,
            dst_ref=hy.at[y],
            send_sem=hys.at[d - 1],
            recv_sem=hyr.at[d - 1],
            device_id={"dom": y_at(d)},
            device_id_type=MESH,
        )
        copy.start()
        hub_y.append(copy)

    y_copies = {}

    def bulk(h):
        span = slice(h * chunk, (h + 1) * chunk)
        for d in range(1, n_feat):
            x_copies[h, d].wait()
        total = sx[j, h].astype(F32)
        for d in range(1, n_feat):
            total = total + rx[h, d - 1].astype(F32)
        proj = total.astype(BF16)
        for b in range(own_blocks):
            ext_ref[b, span, :] = proj[:, b * BLK : (b + 1) * BLK]
        stacked = jnp.concatenate([proj[:, g * LO : (g + 1) * LO] for g in range(his)], 0)
        for s in SEND_ORDER:
            hi = lax.div(send_ref[s : s + 1, :], LO)
            rows_out = pick_groups(dot(stacked, hot_ref[s]), hi, his, chunk).astype(BF16)
            for b in range(slot_blocks):
                sy[h, s, b] = rows_out[:, b * BLK : (b + 1) * BLK]
            first = own_blocks + s * slot_blocks
            y_copies[h, s] = pltpu.make_async_remote_copy(
                src_ref=sy.at[h, s],
                dst_ref=ext_ref.at[first : first + slot_blocks, span, :],
                send_sem=sys_.at[h, s],
                recv_sem=syr.at[h, s],
                device_id={"dom": p + OFFSETS[s]},
                device_id_type=MESH,
            )

            @pl.when(inside(OFFSETS[s]))
            def _():
                y_copies[h, s].start()

    bulk(0)

    for copy in hub_y:
        copy.wait()
    arrived = [hy[source].astype(F32) for source in range(Y_RING)]
    for t in range(packed // BLK):
        lane = lax.broadcasted_iota(I32, (half, BLK), 1) + t * BLK
        low_tile = jnp.zeros((half, BLK), F32)
        high_tile = jnp.zeros((half, BLK), F32)
        for source in range(Y_RING):
            low, high = source * HUB_MOST, (source + 1) * HUB_MOST
            if high <= t * BLK or low >= (t + 1) * BLK:
                continue
            here = (lane >= low) & (lane < high)
            low_tile = jnp.where(here, arrived[source], low_tile)
            high_tile = jnp.where(here, pltpu.roll(arrived[source], BLK // 2, 1), high_tile)
        hpack[:half, t * BLK : (t + 1) * BLK] = low_tile.astype(BF16)
        hpack[half:, t * BLK : (t + 1) * BLK] = high_tile.astype(BF16)
    hz[z] = hpack[...]

    @pl.when(j == ring_desk)
    def _():
        pl.semaphore_wait(barrier, z_ring - 1)
        for other in range(n_feat):
            if other != ring_desk:
                tell(ring_in, p, other)

    @pl.when(j != ring_desk)
    def _():
        pl.semaphore_wait(ring_in, 1)

    hub_z = []
    for d in range(1, z_ring):
        copy = pltpu.make_async_remote_copy(
            src_ref=hpack,
            dst_ref=hz.at[z],
            send_sem=hzs.at[d - 1],
            recv_sem=hzr.at[d - 1],
            device_id={"dom": z_at(d)},
            device_id_type=MESH,
        )
        copy.start()
        hub_z.append(copy)

    for h in range(1, n_chunk):
        bulk(h)

    for copy in hub_z:
        copy.wait()
    everyone = jnp.concatenate([hz[source] for source in range(z_ring)], 0)
    hub_block = pick_groups(dot(everyone, endhot_ref[...]), end_z, z_ring, cols).astype(BF16)
    for b in range(hubs // BLK):
        ext_ref[hub_first + b] = hub_block[:, b * BLK : (b + 1) * BLK]

    loads[8].wait()
    for (h, s), copy in y_copies.items():

        @pl.when(inside(OFFSETS[s]))
        def _():
            copy.wait_send()

        @pl.when(inside(-OFFSETS[s]))
        def _():
            copy.wait_recv()


def tile_kernel(meta_ref, tiles_ref, ext_ref, bias_ref, out_ref, acc_ref):
    row_blocks = acc_ref.shape[0] - 1
    acc_ref[...] = jnp.zeros_like(acc_ref)
    unroll = 36
    columns = ext_ref.shape[1]

    @pl.loop(0, tiles_ref.shape[0] // unroll)
    def _(step):
        products = []
        for u in range(0, unroll, 2):
            t = step * unroll + u
            left = jnp.concatenate([ext_ref[meta_ref[1, t]], ext_ref[meta_ref[1, t + 1]]], 0)
            both = dot(left, tiles_ref[pl.ds(t, 2)].reshape(2 * BLK, BLK), 1, 1)
            products += [both[:columns, :BLK], both[columns:, BLK:]]
        for u in range(unroll):
            acc_ref[meta_ref[0, step * unroll + u]] += products[u]

    bias = bias_ref[...]
    for b in range(row_blocks):
        out_ref[:, b * BLK : (b + 1) * BLK] = jnp.maximum(acc_ref[b] + bias, 0.0).astype(BF16)


def local(
    n_dom, n_feat,
    features, weight, out_bias, tile_values, tile_rows, tile_cols, tile_count, send_rows, hub_ids,
):
    rows, _ = features.shape
    cols = out_bias.shape[0]
    hubs = hub_ids.shape[0]
    slots, halo = send_rows.shape[1:]
    chunk = 8
    n_chunk = cols // chunk
    z_ring = n_dom // Y_RING
    blocks = (rows + slots * halo + hubs) // BLK
    vmem = pl.BlockSpec(memory_space=pltpu.VMEM)
    dma = pltpu.SemaphoreType.DMA
    tiles = tile_values.shape[0]
    shape = jax.ShapeDtypeStruct
    carried = 2 * blocks * cols * BLK + 2 * tile_values.size + 4 * (8 + cols) * BLK
    extended, held_tiles, meta, bias = pl.pallas_call(
        functools.partial(exchange_kernel, n_dom, n_feat, cols, chunk),
        out_shape=(
            pltpu.VMEM((blocks, cols, BLK), BF16),
            pltpu.VMEM(tile_values.shape, BF16),
            pltpu.VMEM((8, BLK), I32),
            pltpu.VMEM((cols, BLK), F32),
        ),
        in_specs=[pl.BlockSpec(memory_space=pltpu.HBM)] * 9,
        out_specs=(vmem,) * 4,
        scratch_shapes=[
            pltpu.VMEM((features.shape[1], rows), BF16),
            pltpu.VMEM(weight.shape, BF16),
            pltpu.VMEM((slots, halo), I32),
            pltpu.VMEM((hubs // BLK, BLK), I32),
            pltpu.VMEM((slots, LO, halo), BF16),
            pltpu.VMEM((Y_RING * HUB_MOST, hubs), BF16),
            pltpu.VMEM((n_feat, n_chunk, chunk, rows), BF16),
            pltpu.VMEM((n_chunk, n_feat - 1, chunk, rows), BF16),
            pltpu.VMEM((n_chunk, slots, halo // BLK, chunk, BLK), BF16),
            pltpu.VMEM((n_feat, cols // 2, BLK), BF16),
            pltpu.VMEM((n_feat - 1, cols // 2, BLK), BF16),
            pltpu.VMEM((cols // 2, BLK), BF16),
            pltpu.VMEM((Y_RING, cols // 2, BLK), BF16),
            pltpu.VMEM((cols, Y_RING * HUB_MOST), BF16),
            pltpu.VMEM((z_ring, cols, Y_RING * HUB_MOST), BF16),
            pltpu.VMEM((2, 1, tiles), I32),
            pltpu.SMEM((1,), I32),
            pltpu.VMEM((1, cols), F32),
            dma((9,)),
            dma((n_chunk, n_feat - 1)),
            dma((n_chunk, n_feat - 1)),
            dma((n_chunk, slots)),
            dma((n_chunk, slots)),
            dma((n_feat - 1,)),
            dma((n_feat - 1,)),
            dma((Y_RING - 1,)),
            dma((Y_RING - 1,)),
            dma((z_ring - 1,)),
            dma((z_ring - 1,)),
            pltpu.SemaphoreType.REGULAR,
            pltpu.SemaphoreType.REGULAR,
            pltpu.SemaphoreType.REGULAR,
        ],
        compiler_params=pltpu.CompilerParams(
            collective_id=0,
            has_side_effects=True,
            vmem_limit_bytes=VMEM_MOST - carried - 65536,
        ),
        name="exchange",
    )(
        features.T, weight, send_rows[0], hub_ids.reshape(hubs // BLK, BLK), tile_values,
        tile_rows[None, :], tile_cols[None, :], tile_count, out_bias[None, :],
    )
    out_t = pl.pallas_call(
        tile_kernel,
        out_shape=shape((cols, rows), BF16),
        in_specs=[pl.BlockSpec(memory_space=pltpu.SMEM), vmem, vmem, vmem],
        out_specs=vmem,
        scratch_shapes=[pltpu.VMEM((rows // BLK + 1, cols, BLK), F32)],
        compiler_params=pltpu.CompilerParams(vmem_limit_bytes=16 * 2**20),
        name="tiles",
    )(meta, held_tiles, extended, bias)
    return out_t.T


def solution(mesh):
    in_specs = (
        P("dom", "feat"),
        P(),
        P("feat"),
        P("dom", None, None),
        P("dom"),
        P("dom"),
        P("dom"),
        P("dom", None, None),
        P(),
    )
    out_specs = P("dom", "feat")
    body = functools.partial(local, mesh.shape["dom"], mesh.shape["feat"])
    return jax.shard_map(body, mesh=mesh, in_specs=in_specs, out_specs=out_specs, check_vma=False)
```

```python
import functools

import jax
import jax.numpy as jnp
from jax import lax
from jax.experimental import pallas as pl
from jax.experimental.pallas import tpu as pltpu
from jax.sharding import PartitionSpec as P

REACH = 4
HUB_MOST = 48
Y_RING = 8
LO = 256
BLK = 128
OFFSETS = tuple(range(-REACH, 0)) + tuple(range(1, REACH + 1))
SEND_ORDER = (0, 7, 1, 6, 2, 5, 3, 4)
VMEM_MOST = 67_043_328
MESH = pl.DeviceIdType.MESH
F32, BF16, I32 = jnp.float32, jnp.bfloat16, jnp.int32


def dims(a, b):
    return (((a,), (b,)), ((), ()))


def dot(a, b, ca=1, cb=0):
    return lax.dot_general(a, b, dims(ca, cb), preferred_element_type=F32)


def ones_where(mask):
    return jnp.where(mask, 1.0, 0.0).astype(BF16)


def ascending(shape, swap=False):
    a, b = lax.broadcasted_iota(I32, shape, 0), lax.broadcasted_iota(I32, shape, 1)
    return b < a if swap else a < b


def pick_groups(stacked, group_of, groups, height):
    total = jnp.zeros((height, stacked.shape[1]), F32)
    for g in range(groups):
        total = jnp.where(group_of == g, stacked[g * height : (g + 1) * height], total)
    return total


def arrived_in(ref, sem):
    pltpu.make_async_copy(ref, ref, sem).wait()


def as_row(x):
    return jnp.concatenate([x[i : i + 1] for i in range(x.shape[0])], 1)


def exchange_kernel(
    n_dom, n_feat, cols, chunk,
    ft_hbm, w_hbm, send_hbm, hub_hbm, tiles_hbm, rows_hbm, cols_hbm, count_hbm, bias_hbm,
    ext_ref, tiles_ref, meta_ref, bias_ref,
    ft_ref, w_ref, send_ref, hub_ref, hot_ref, endhot_ref, sx, rx, sy,
    hx_out, hx, hub_out, hy, hpack, hz, meta_in, count_in, bias_in,
    in_sem, sxs, sxr, sys_, syr, hxs, hxr, hys, hyr, hzs, hzr, feat_in, near_in, ring_in,
):
    p = lax.axis_index("dom")
    j = lax.axis_index("feat")
    y = lax.rem(p, Y_RING)
    z = lax.div(p, Y_RING)
    z_ring = n_dom // Y_RING
    k_in, rows = ft_ref.shape
    n_chunk = cols // chunk
    his = rows // LO
    slots, halo = send_ref.shape
    own_blocks = rows // BLK
    slot_blocks = halo // BLK
    hub_first = own_blocks + slots * slot_blocks
    near_desk, ring_desk = n_feat - 1, n_feat - 2

    loads = []
    for i, (src, dst) in enumerate(
        (
            (hub_hbm, hub_ref), (ft_hbm, ft_ref), (w_hbm, w_ref), (send_hbm, send_ref),
            (rows_hbm, meta_in.at[0]), (cols_hbm, meta_in.at[1]),
            (count_hbm, count_in), (bias_hbm, bias_in), (tiles_hbm, tiles_ref),
        )
    ):
        loads.append(pltpu.make_async_copy(src, dst, in_sem.at[i]))
        loads[-1].start()

    def y_at(step):
        return z * Y_RING + lax.rem(y + step, Y_RING)

    def z_at(step):
        return lax.rem(z + step, z_ring) * Y_RING + y

    def feat_at(step):
        return lax.rem(j + step, n_feat)

    def tell(sem, dom, feat):
        pl.semaphore_signal(
            sem, inc=1, device_id={"dom": dom, "feat": feat}, device_id_type=MESH
        )

    def inside(o):
        return (p + o >= 0) & (p + o < n_dom)

    barrier = pltpu.get_barrier_semaphore()
    for other in range(ring_desk):

        @pl.when(j != other)
        def _():
            tell(barrier, p, other)

    loads[0].wait()

    ids = hub_ref[...]
    hubs = ids.size
    mine = lax.div(ids, rows) == p
    mine_ones = ones_where(mine)
    side = ids.shape[0]
    in_row = dot(mine_ones, ones_where(ascending((BLK, BLK))))
    above = jnp.sum(dot(ones_where(ascending((side, side), True)), mine_ones), 1, keepdims=True)
    my_rank = (in_row + above).astype(I32)
    local_row = lax.rem(ids, rows)
    place = as_row(jnp.where(mine, lax.rem(my_rank + y * HUB_MOST, BLK), -1))
    taken = ones_where(lax.broadcasted_iota(I32, (BLK, hubs), 0) == place)
    halves = jnp.concatenate(
        [as_row(lax.rem(local_row, LO).astype(F32)), as_row((lax.div(local_row, LO) + 1).astype(F32))]
        + [jnp.zeros((14, hubs), F32)],
        0,
    ).astype(BF16)
    listed = dot(halves, taken, 1, 1)
    hub_row = (listed[0:1] + LO * (listed[1:2] - 1.0)).astype(I32)
    hub_pick = ones_where(lax.broadcasted_iota(I32, (rows, BLK), 0) == hub_row)

    f_in = w_ref.shape[0]
    loads[2].wait()
    pick = ones_where(
        lax.broadcasted_iota(I32, (BLK, f_in), 1)
        == lax.broadcasted_iota(I32, (BLK, f_in), 0) + j * k_in
    )
    w_mine = dot(pick, w_ref[...])
    w_t = w_mine.T.astype(BF16)[:, :k_in]

    loads[1].wait()
    ft = ft_ref[...]
    hub_ft = dot(ft, hub_pick).astype(BF16)
    hub_part = dot(w_t, hub_ft)
    half = cols // 2
    for d in range(n_feat):
        lower = hub_part[d * cols : d * cols + half]
        upper = hub_part[d * cols + half : (d + 1) * cols]
        hx_out[d] = (lower + pltpu.roll(upper, BLK // 2, 1)).astype(BF16)

    @pl.when(j < ring_desk)
    def _():
        pl.semaphore_wait(barrier, n_feat - 1)

    @pl.when(j == 0)
    def _():
        tell(feat_in, p, near_desk)
        tell(feat_in, p, ring_desk)

    @pl.when(j >= ring_desk)
    def _():
        pl.semaphore_wait(feat_in, 1)

    @pl.when(j == near_desk)
    def _():
        for o in OFFSETS:

            @pl.when(inside(o))
            def _():
                tell(barrier, p + o, near_desk)

        for d in range(1, Y_RING):
            tell(barrier, y_at(d), near_desk)

    @pl.when(j == ring_desk)
    def _():
        for d in range(1, z_ring):
            tell(barrier, z_at(d), ring_desk)

    for d in range(1, n_feat):
        copy = pltpu.make_async_remote_copy(
            src_ref=hx_out.at[feat_at(d)],
            dst_ref=hx.at[d - 1],
            send_sem=hxs,
            recv_sem=hxr,
            device_id={"feat": feat_at(d)},
            device_id_type=MESH,
        )
        copy.start()

    for h in range(n_chunk):
        left = jnp.concatenate(
            [w_t[d * cols + h * chunk : d * cols + (h + 1) * chunk] for d in range(n_feat)], 0
        )
        part = dot(left, ft).astype(BF16)
        for d in range(n_feat):
            sx[d, h] = part[d * chunk : (d + 1) * chunk]
        for d in range(1, n_feat):
            copy = pltpu.make_async_remote_copy(
                src_ref=sx.at[feat_at(d), h],
                dst_ref=rx.at[h, d - 1],
                send_sem=sxs,
                recv_sem=sxr.at[h],
                device_id={"feat": feat_at(d)},
                device_id_type=MESH,
            )
            copy.start()

    loads[3].wait()
    for s in range(slots):
        lo = lax.rem(send_ref[s : s + 1, :], LO)
        hot_ref[s] = ones_where(lax.broadcasted_iota(I32, (LO, halo), 0) == lo)
    packed = Y_RING * HUB_MOST
    ids_row = as_row(ids)
    owner = lax.div(ids_row, rows)
    owned = lax.broadcasted_iota(I32, (n_dom, hubs), 0) == owner
    earlier = dot(ones_where(owned), ones_where(ascending((hubs, hubs))))
    rank = jnp.sum(jnp.where(owned, earlier, 0.0), 0, keepdims=True).astype(I32)
    end_place = lax.rem(owner, Y_RING) * HUB_MOST + rank
    end_z = lax.div(owner, Y_RING)
    endhot_ref[...] = ones_where(lax.broadcasted_iota(I32, (packed, hubs), 0) == end_place)

    for i in range(4, 8):
        loads[i].wait()
    tiles = meta_in.shape[2]
    live = lax.broadcasted_iota(I32, (1, tiles), 1) < count_in[0]
    meta_ref[0:1, 0:tiles] = jnp.where(live, meta_in[0], own_blocks)
    meta_ref[1:2, 0:tiles] = meta_in[1]
    eye = lax.broadcasted_iota(I32, (cols, cols), 0) == lax.broadcasted_iota(I32, (cols, cols), 1)
    bias = jnp.sum(jnp.where(eye, bias_in[...], 0.0), 1, keepdims=True)
    bias_ref[...] = jnp.broadcast_to(bias, (cols, BLK))

    for s in range(slots):

        @pl.when(jnp.logical_not(inside(-OFFSETS[s])))
        def _():
            first = own_blocks + s * slot_blocks
            ext_ref[first : first + slot_blocks] = jnp.zeros((slot_blocks, cols, BLK), BF16)

    arrived_in(hx, hxr)
    hub_sum = hx_out[j].astype(F32)
    for d in range(1, n_feat):
        hub_sum = hub_sum + hx[d - 1].astype(F32)
    hub_mine = hub_sum.astype(BF16)
    hub_out[...] = hub_mine
    hy[y] = hub_mine

    @pl.when(j == near_desk)
    def _():
        before_p = lax.min(p, REACH)
        after_p = lax.min(n_dom - 1 - p, REACH)
        pl.semaphore_wait(barrier, before_p + after_p + Y_RING - 1)
        for other in range(n_feat - 1):
            tell(near_in, p, other)

    @pl.when(j != near_desk)
    def _():
        pl.semaphore_wait(near_in, 1)

    for d in range(1, Y_RING):
        copy = pltpu.make_async_remote_copy(
            src_ref=hub_out,
            dst_ref=hy.at[y],
            send_sem=hys,
            recv_sem=hyr,
            device_id={"dom": y_at(d)},
            device_id_type=MESH,
        )
        copy.start()

    def bulk(h):
        span = slice(h * chunk, (h + 1) * chunk)
        arrived_in(rx.at[h], sxr.at[h])
        total = sx[j, h].astype(F32)
        for d in range(1, n_feat):
            total = total + rx[h, d - 1].astype(F32)
        proj = total.astype(BF16)
        for b in range(own_blocks):
            ext_ref[b, span, :] = proj[:, b * BLK : (b + 1) * BLK]
        stacked = jnp.concatenate([proj[:, g * LO : (g + 1) * LO] for g in range(his)], 0)
        for s in SEND_ORDER:
            hi = lax.div(send_ref[s : s + 1, :], LO)
            rows_out = pick_groups(dot(stacked, hot_ref[s]), hi, his, chunk).astype(BF16)
            for b in range(slot_blocks):
                sy[h, s, b] = rows_out[:, b * BLK : (b + 1) * BLK]
            first = own_blocks + s * slot_blocks
            copy = pltpu.make_async_remote_copy(
                src_ref=sy.at[h, s],
                dst_ref=ext_ref.at[first : first + slot_blocks, span, :],
                send_sem=sys_.at[s],
                recv_sem=syr.at[s],
                device_id={"dom": p + OFFSETS[s]},
                device_id_type=MESH,
            )

            @pl.when(inside(OFFSETS[s]))
            def _():
                copy.start()

    bulk(0)
    bulk(1)

    arrived_in(hy.at[0 : Y_RING - 1], hyr)
    arrived = [hy[source].astype(F32) for source in range(Y_RING)]
    for t in range(packed // BLK):
        lane = lax.broadcasted_iota(I32, (half, BLK), 1) + t * BLK
        low_tile = jnp.zeros((half, BLK), F32)
        high_tile = jnp.zeros((half, BLK), F32)
        for source in range(Y_RING):
            low, high = source * HUB_MOST, (source + 1) * HUB_MOST
            if high <= t * BLK or low >= (t + 1) * BLK:
                continue
            here = (lane >= low) & (lane < high)
            low_tile = jnp.where(here, arrived[source], low_tile)
            high_tile = jnp.where(here, pltpu.roll(arrived[source], BLK // 2, 1), high_tile)
        hpack[:half, t * BLK : (t + 1) * BLK] = low_tile.astype(BF16)
        hpack[half:, t * BLK : (t + 1) * BLK] = high_tile.astype(BF16)
    hz[z] = hpack[...]

    @pl.when(j == ring_desk)
    def _():
        pl.semaphore_wait(barrier, z_ring - 1)
        for other in range(n_feat):
            if other != ring_desk:
                tell(ring_in, p, other)

    @pl.when(j != ring_desk)
    def _():
        pl.semaphore_wait(ring_in, 1)

    for d in range(1, z_ring):
        copy = pltpu.make_async_remote_copy(
            src_ref=hpack,
            dst_ref=hz.at[z],
            send_sem=hzs,
            recv_sem=hzr,
            device_id={"dom": z_at(d)},
            device_id_type=MESH,
        )
        copy.start()

    for h in range(2, n_chunk):
        bulk(h)

    arrived_in(hz.at[0 : z_ring - 1], hzr)
    everyone = jnp.concatenate([hz[source] for source in range(z_ring)], 0)
    hub_block = pick_groups(dot(everyone, endhot_ref[...]), end_z, z_ring, cols).astype(BF16)
    for b in range(hubs // BLK):
        ext_ref[hub_first + b] = hub_block[:, b * BLK : (b + 1) * BLK]

    loads[8].wait()
    for s in range(slots):
        first = own_blocks + s * slot_blocks
        slot_rows = ext_ref.at[first : first + slot_blocks]

        @pl.when(inside(-OFFSETS[s]))
        def _():
            arrived_in(slot_rows, syr.at[s])

        @pl.when(inside(OFFSETS[s]))
        def _():
            arrived_in(slot_rows, sys_.at[s])

    arrived_in(hx, hxs)
    arrived_in(rx, sxs)
    arrived_in(hy.at[0 : Y_RING - 1], hys)
    arrived_in(hz.at[0 : z_ring - 1], hzs)


def tile_kernel(meta_ref, tiles_ref, ext_ref, bias_ref, out_ref, acc_ref):
    row_blocks = acc_ref.shape[0] - 1
    acc_ref[...] = jnp.zeros_like(acc_ref)
    unroll = 36
    columns = ext_ref.shape[1]

    @pl.loop(0, tiles_ref.shape[0] // unroll)
    def _(step):
        products = []
        for u in range(0, unroll, 2):
            t = step * unroll + u
            left = jnp.concatenate([ext_ref[meta_ref[1, t]], ext_ref[meta_ref[1, t + 1]]], 0)
            both = dot(left, tiles_ref[pl.ds(t, 2)].reshape(2 * BLK, BLK), 1, 1)
            products += [both[:columns, :BLK], both[columns:, BLK:]]
        for u in range(unroll):
            acc_ref[meta_ref[0, step * unroll + u]] += products[u]

    bias = bias_ref[...]
    for b in range(row_blocks):
        out_ref[:, b * BLK : (b + 1) * BLK] = jnp.maximum(acc_ref[b] + bias, 0.0).astype(BF16)


def local(
    n_dom, n_feat,
    features, weight, out_bias, tile_values, tile_rows, tile_cols, tile_count, send_rows, hub_ids,
):
    rows, _ = features.shape
    cols = out_bias.shape[0]
    hubs = hub_ids.shape[0]
    slots, halo = send_rows.shape[1:]
    chunk = 8
    n_chunk = cols // chunk
    z_ring = n_dom // Y_RING
    blocks = (rows + slots * halo + hubs) // BLK
    vmem = pl.BlockSpec(memory_space=pltpu.VMEM)
    dma = pltpu.SemaphoreType.DMA
    tiles = tile_values.shape[0]
    shape = jax.ShapeDtypeStruct
    carried = 2 * blocks * cols * BLK + 2 * tile_values.size + 4 * (8 + cols) * BLK
    extended, held_tiles, meta, bias = pl.pallas_call(
        functools.partial(exchange_kernel, n_dom, n_feat, cols, chunk),
        out_shape=(
            pltpu.VMEM((blocks, cols, BLK), BF16),
            pltpu.VMEM(tile_values.shape, BF16),
            pltpu.VMEM((8, BLK), I32),
            pltpu.VMEM((cols, BLK), F32),
        ),
        in_specs=[pl.BlockSpec(memory_space=pltpu.HBM)] * 9,
        out_specs=(vmem,) * 4,
        scratch_shapes=[
            pltpu.VMEM((features.shape[1], rows), BF16),
            pltpu.VMEM(weight.shape, BF16),
            pltpu.VMEM((slots, halo), I32),
            pltpu.VMEM((hubs // BLK, BLK), I32),
            pltpu.VMEM((slots, LO, halo), BF16),
            pltpu.VMEM((Y_RING * HUB_MOST, hubs), BF16),
            pltpu.VMEM((n_feat, n_chunk, chunk, rows), BF16),
            pltpu.VMEM((n_chunk, n_feat - 1, chunk, rows), BF16),
            pltpu.VMEM((n_chunk, slots, halo // BLK, chunk, BLK), BF16),
            pltpu.VMEM((n_feat, cols // 2, BLK), BF16),
            pltpu.VMEM((n_feat - 1, cols // 2, BLK), BF16),
            pltpu.VMEM((cols // 2, BLK), BF16),
            pltpu.VMEM((Y_RING, cols // 2, BLK), BF16),
            pltpu.VMEM((cols, Y_RING * HUB_MOST), BF16),
            pltpu.VMEM((z_ring, cols, Y_RING * HUB_MOST), BF16),
            pltpu.VMEM((2, 1, tiles), I32),
            pltpu.SMEM((1,), I32),
            pltpu.VMEM((1, cols), F32),
            dma((9,)),
            dma,
            dma((n_chunk,)),
            dma((slots,)),
            dma((slots,)),
            dma,
            dma,
            dma,
            dma,
            dma,
            dma,
            pltpu.SemaphoreType.REGULAR,
            pltpu.SemaphoreType.REGULAR,
            pltpu.SemaphoreType.REGULAR,
        ],
        compiler_params=pltpu.CompilerParams(
            collective_id=0,
            has_side_effects=True,
            vmem_limit_bytes=VMEM_MOST - carried - 65536,
        ),
        name="exchange",
    )(
        features.T, weight, send_rows[0], hub_ids.reshape(hubs // BLK, BLK), tile_values,
        tile_rows[None, :], tile_cols[None, :], tile_count, out_bias[None, :],
    )
    out_t = pl.pallas_call(
        tile_kernel,
        out_shape=shape((cols, rows), BF16),
        in_specs=[pl.BlockSpec(memory_space=pltpu.SMEM), vmem, vmem, vmem],
        out_specs=vmem,
        scratch_shapes=[pltpu.VMEM((rows // BLK + 1, cols, BLK), F32)],
        compiler_params=pltpu.CompilerParams(vmem_limit_bytes=16 * 2**20),
        name="tiles",
    )(meta, held_tiles, extended, bias)
    return out_t.T


def solution(mesh):
    in_specs = (
        P("dom", "feat"),
        P(),
        P("feat"),
        P("dom", None, None),
        P("dom"),
        P("dom"),
        P("dom"),
        P("dom", None, None),
        P(),
    )
    out_specs = P("dom", "feat")
    body = functools.partial(local, mesh.shape["dom"], mesh.shape["feat"])
    return jax.shard_map(body, mesh=mesh, in_specs=in_specs, out_specs=out_specs, check_vma=False)
```

```python
import functools

import jax
import jax.numpy as jnp
from jax import lax
from jax.experimental import pallas as pl
from jax.experimental.pallas import tpu as pltpu
from jax.sharding import PartitionSpec as P

REACH = 4
HUB_MOST = 48
Y_RING = 8
LO = 256
BLK = 128
OFFSETS = tuple(range(-REACH, 0)) + tuple(range(1, REACH + 1))
SEND_ORDER = (0, 7, 1, 6, 2, 5, 3, 4)
VMEM_MOST = 67_043_328
MESH = pl.DeviceIdType.MESH
F32, BF16, I32 = jnp.float32, jnp.bfloat16, jnp.int32


def dims(a, b):
    return (((a,), (b,)), ((), ()))


def dot(a, b, ca=1, cb=0):
    return lax.dot_general(a, b, dims(ca, cb), preferred_element_type=F32)


def ones_where(mask):
    return jnp.where(mask, 1.0, 0.0).astype(BF16)


def ascending(shape, swap=False):
    a, b = lax.broadcasted_iota(I32, shape, 0), lax.broadcasted_iota(I32, shape, 1)
    return b < a if swap else a < b


def pick_groups(stacked, group_of, groups, height):
    total = jnp.zeros((height, stacked.shape[1]), F32)
    for g in range(groups):
        total = jnp.where(group_of == g, stacked[g * height : (g + 1) * height], total)
    return total


def arrived_in(ref, sem):
    pltpu.make_async_copy(ref, ref, sem).wait()


def as_row(x):
    return jnp.concatenate([x[i : i + 1] for i in range(x.shape[0])], 1)


def exchange_kernel(
    n_dom, n_feat, cols, chunk,
    ft_hbm, w_hbm, send_hbm, hub_hbm, tiles_hbm, rows_hbm, cols_hbm, count_hbm, bias_hbm,
    ext_ref, tiles_ref, meta_smem, bias_ref,
    ft_ref, w_ref, send_ref, hub_ref, hot_ref, endhot_ref, sx, rx, sy,
    hx_out, hx, hub_out, hy, hpack, hz, meta_in, meta_ref, count_in, bias_in,
    in_sem, sxs, sxr, sys_, syr, hxs, hxr, hys, hyr, hzs, hzr, feat_in, near_in, ring_in,
):
    p = lax.axis_index("dom")
    j = lax.axis_index("feat")
    y = lax.rem(p, Y_RING)
    z = lax.div(p, Y_RING)
    z_ring = n_dom // Y_RING
    k_in, rows = ft_ref.shape
    n_chunk = cols // chunk
    his = rows // LO
    slots, halo = send_ref.shape
    own_blocks = rows // BLK
    slot_blocks = halo // BLK
    hub_first = own_blocks + slots * slot_blocks
    near_desk, ring_desk = n_feat - 1, n_feat - 3
    desks = (near_desk, ring_desk)
    at_desk = (j == near_desk) | (j == ring_desk)

    loads = []
    for i, (src, dst) in enumerate(
        (
            (hub_hbm, hub_ref), (ft_hbm, ft_ref), (w_hbm, w_ref), (send_hbm, send_ref),
            (rows_hbm, meta_in.at[0]), (cols_hbm, meta_in.at[1]),
            (count_hbm, count_in), (bias_hbm, bias_in), (tiles_hbm, tiles_ref),
        )
    ):
        loads.append(pltpu.make_async_copy(src, dst, in_sem.at[i]))
        loads[-1].start()

    def y_at(step):
        return z * Y_RING + lax.rem(y + step, Y_RING)

    def z_at(step):
        return lax.rem(z + step, z_ring) * Y_RING + y

    def feat_at(step):
        return lax.rem(j + step, n_feat)

    def tell(sem, dom, feat):
        pl.semaphore_signal(
            sem, inc=1, device_id={"dom": dom, "feat": feat}, device_id_type=MESH
        )

    def inside(o):
        return (p + o >= 0) & (p + o < n_dom)

    barrier = pltpu.get_barrier_semaphore()
    for other in range(n_feat):
        if other in desks:
            continue

        @pl.when(j != other)
        def _():
            tell(barrier, p, other)

    loads[0].wait()

    ids = hub_ref[...]
    hubs = ids.size
    mine = lax.div(ids, rows) == p
    mine_ones = ones_where(mine)
    side = ids.shape[0]
    in_row = dot(mine_ones, ones_where(ascending((BLK, BLK))))
    above = jnp.sum(dot(ones_where(ascending((side, side), True)), mine_ones), 1, keepdims=True)
    my_rank = (in_row + above).astype(I32)
    local_row = lax.rem(ids, rows)
    place = as_row(jnp.where(mine, lax.rem(my_rank + y * HUB_MOST, BLK), -1))
    taken = ones_where(lax.broadcasted_iota(I32, (BLK, hubs), 0) == place)
    halves = jnp.concatenate(
        [as_row(lax.rem(local_row, LO).astype(F32)), as_row((lax.div(local_row, LO) + 1).astype(F32))]
        + [jnp.zeros((14, hubs), F32)],
        0,
    ).astype(BF16)
    listed = dot(halves, taken, 1, 1)
    hub_row = (listed[0:1] + LO * (listed[1:2] - 1.0)).astype(I32)
    hub_pick = ones_where(lax.broadcasted_iota(I32, (rows, BLK), 0) == hub_row)

    f_in = w_ref.shape[0]
    loads[2].wait()
    pick = ones_where(
        lax.broadcasted_iota(I32, (BLK, f_in), 1)
        == lax.broadcasted_iota(I32, (BLK, f_in), 0) + j * k_in
    )
    w_mine = dot(pick, w_ref[...])
    w_t = w_mine.T.astype(BF16)[:, :k_in]

    loads[1].wait()
    ft = ft_ref[...]
    hub_ft = dot(ft, hub_pick).astype(BF16)
    hub_part = dot(w_t, hub_ft)
    half = cols // 2
    for d in range(n_feat):
        lower = hub_part[d * cols : d * cols + half]
        upper = hub_part[d * cols + half : (d + 1) * cols]
        hx_out[d] = (lower + pltpu.roll(upper, BLK // 2, 1)).astype(BF16)

    @pl.when(jnp.logical_not(at_desk))
    def _():
        pl.semaphore_wait(barrier, n_feat - 1)

    for desk in desks:

        @pl.when(j == desk - 1)
        def _():
            tell(feat_in, p, desk)

    @pl.when(at_desk)
    def _():
        pl.semaphore_wait(feat_in, 1)

    @pl.when(j == near_desk)
    def _():
        for o in OFFSETS:

            @pl.when(inside(o))
            def _():
                tell(barrier, p + o, near_desk)

        for d in range(1, Y_RING):
            tell(barrier, y_at(d), near_desk)

    @pl.when(j == ring_desk)
    def _():
        for d in range(1, z_ring):
            tell(barrier, z_at(d), ring_desk)

    for d in range(1, n_feat):
        copy = pltpu.make_async_remote_copy(
            src_ref=hx_out.at[feat_at(d)],
            dst_ref=hx.at[d - 1],
            send_sem=hxs,
            recv_sem=hxr,
            device_id={"feat": feat_at(d)},
            device_id_type=MESH,
        )
        copy.start()

    for h in range(n_chunk):
        left = jnp.concatenate(
            [w_t[d * cols + h * chunk : d * cols + (h + 1) * chunk] for d in range(n_feat)], 0
        )
        part = dot(left, ft).astype(BF16)
        for d in range(n_feat):
            sx[d, h] = part[d * chunk : (d + 1) * chunk]
        for d in range(1, n_feat):
            copy = pltpu.make_async_remote_copy(
                src_ref=sx.at[feat_at(d), h],
                dst_ref=rx.at[h, d - 1],
                send_sem=sxs,
                recv_sem=sxr.at[h],
                device_id={"feat": feat_at(d)},
                device_id_type=MESH,
            )
            copy.start()

    loads[3].wait()
    for s in range(slots):
        lo = lax.rem(send_ref[s : s + 1, :], LO)
        hot_ref[s] = ones_where(lax.broadcasted_iota(I32, (LO, halo), 0) == lo)
    packed = Y_RING * HUB_MOST
    ids_row = as_row(ids)
    owner = lax.div(ids_row, rows)
    owned = lax.broadcasted_iota(I32, (n_dom, hubs), 0) == owner
    earlier = dot(ones_where(owned), ones_where(ascending((hubs, hubs))))
    rank = jnp.sum(jnp.where(owned, earlier, 0.0), 0, keepdims=True).astype(I32)
    end_place = lax.rem(owner, Y_RING) * HUB_MOST + rank
    end_z = lax.div(owner, Y_RING)
    endhot_ref[...] = ones_where(lax.broadcasted_iota(I32, (packed, hubs), 0) == end_place)

    for i in range(4, 8):
        loads[i].wait()
    tiles = meta_in.shape[2]
    live = lax.broadcasted_iota(I32, (1, tiles), 1) < count_in[0]
    meta_ref[0:1, 0:tiles] = jnp.where(live, meta_in[0], own_blocks)
    meta_ref[1:2, 0:tiles] = meta_in[1]
    hand_over = pltpu.make_async_copy(meta_ref, meta_smem, in_sem.at[4])
    hand_over.start()
    eye = lax.broadcasted_iota(I32, (cols, cols), 0) == lax.broadcasted_iota(I32, (cols, cols), 1)
    bias = jnp.sum(jnp.where(eye, bias_in[...], 0.0), 1, keepdims=True)
    bias_ref[...] = jnp.broadcast_to(bias, (cols, BLK))

    for s in range(slots):

        @pl.when(jnp.logical_not(inside(-OFFSETS[s])))
        def _():
            first = own_blocks + s * slot_blocks
            ext_ref[first : first + slot_blocks] = jnp.zeros((slot_blocks, cols, BLK), BF16)

    @pl.when(j == near_desk)
    def _():
        before_p = lax.min(p, REACH)
        after_p = lax.min(n_dom - 1 - p, REACH)
        pl.semaphore_wait(barrier, before_p + after_p + Y_RING - 1)
        for other in range(n_feat - 1):
            tell(near_in, p, other)

    arrived_in(hx, hxr)
    hub_sum = hx_out[j].astype(F32)
    for d in range(1, n_feat):
        hub_sum = hub_sum + hx[d - 1].astype(F32)
    hub_mine = hub_sum.astype(BF16)
    hub_out[...] = hub_mine
    hy[y] = hub_mine

    @pl.when(j != near_desk)
    def _():
        pl.semaphore_wait(near_in, 1)

    for d in range(1, Y_RING):
        copy = pltpu.make_async_remote_copy(
            src_ref=hub_out,
            dst_ref=hy.at[y],
            send_sem=hys,
            recv_sem=hyr,
            device_id={"dom": y_at(d)},
            device_id_type=MESH,
        )
        copy.start()

    def bulk(h):
        span = slice(h * chunk, (h + 1) * chunk)
        arrived_in(rx.at[h], sxr.at[h])
        total = sx[j, h].astype(F32)
        for d in range(1, n_feat):
            total = total + rx[h, d - 1].astype(F32)
        proj = total.astype(BF16)
        for b in range(own_blocks):
            ext_ref[b, span, :] = proj[:, b * BLK : (b + 1) * BLK]
        stacked = jnp.concatenate([proj[:, g * LO : (g + 1) * LO] for g in range(his)], 0)
        for s in SEND_ORDER:
            hi = lax.div(send_ref[s : s + 1, :], LO)
            rows_out = pick_groups(dot(stacked, hot_ref[s]), hi, his, chunk).astype(BF16)
            for b in range(slot_blocks):
                sy[h, s, b] = rows_out[:, b * BLK : (b + 1) * BLK]
            first = own_blocks + s * slot_blocks
            copy = pltpu.make_async_remote_copy(
                src_ref=sy.at[h, s],
                dst_ref=ext_ref.at[first : first + slot_blocks, span, :],
                send_sem=sys_.at[s],
                recv_sem=syr.at[s],
                device_id={"dom": p + OFFSETS[s]},
                device_id_type=MESH,
            )

            @pl.when(inside(OFFSETS[s]))
            def _():
                copy.start()

    bulk(0)
    bulk(1)

    arrived_in(hy.at[0 : Y_RING - 1], hyr)
    arrived = [hy[source].astype(F32) for source in range(Y_RING)]
    for t in range(packed // BLK):
        lane = lax.broadcasted_iota(I32, (half, BLK), 1) + t * BLK
        low_tile = jnp.zeros((half, BLK), F32)
        high_tile = jnp.zeros((half, BLK), F32)
        for source in range(Y_RING):
            low, high = source * HUB_MOST, (source + 1) * HUB_MOST
            if high <= t * BLK or low >= (t + 1) * BLK:
                continue
            here = (lane >= low) & (lane < high)
            low_tile = jnp.where(here, arrived[source], low_tile)
            high_tile = jnp.where(here, pltpu.roll(arrived[source], BLK // 2, 1), high_tile)
        hpack[:half, t * BLK : (t + 1) * BLK] = low_tile.astype(BF16)
        hpack[half:, t * BLK : (t + 1) * BLK] = high_tile.astype(BF16)
    hz[z] = hpack[...]

    @pl.when(j == ring_desk)
    def _():
        pl.semaphore_wait(barrier, z_ring - 1)
        for other in range(n_feat):
            if other != ring_desk:
                tell(ring_in, p, other)

    @pl.when(j != ring_desk)
    def _():
        pl.semaphore_wait(ring_in, 1)

    for d in range(1, z_ring):
        copy = pltpu.make_async_remote_copy(
            src_ref=hpack,
            dst_ref=hz.at[z],
            send_sem=hzs,
            recv_sem=hzr,
            device_id={"dom": z_at(d)},
            device_id_type=MESH,
        )
        copy.start()

    for h in range(2, n_chunk):
        bulk(h)

    arrived_in(hz.at[0 : z_ring - 1], hzr)
    everyone = jnp.concatenate([hz[source] for source in range(z_ring)], 0)
    hub_block = pick_groups(dot(everyone, endhot_ref[...]), end_z, z_ring, cols).astype(BF16)
    for b in range(hubs // BLK):
        ext_ref[hub_first + b] = hub_block[:, b * BLK : (b + 1) * BLK]

    loads[8].wait()
    hand_over.wait()
    for s in range(slots):
        first = own_blocks + s * slot_blocks
        slot_rows = ext_ref.at[first : first + slot_blocks]

        @pl.when(inside(-OFFSETS[s]))
        def _():
            arrived_in(slot_rows, syr.at[s])

        @pl.when(inside(OFFSETS[s]))
        def _():
            arrived_in(slot_rows, sys_.at[s])

    arrived_in(hx, hxs)
    arrived_in(rx, sxs)
    arrived_in(hy.at[0 : Y_RING - 1], hys)
    arrived_in(hz.at[0 : z_ring - 1], hzs)


def tile_kernel(meta_ref, tiles_ref, ext_ref, bias_ref, out_ref, acc_ref):
    row_blocks = acc_ref.shape[0] - 1
    acc_ref[...] = jnp.zeros_like(acc_ref)
    unroll = 36
    columns = ext_ref.shape[1]

    @pl.loop(0, tiles_ref.shape[0] // unroll)
    def _(step):
        products = []
        for u in range(0, unroll, 2):
            t = step * unroll + u
            left = jnp.concatenate([ext_ref[meta_ref[1, t]], ext_ref[meta_ref[1, t + 1]]], 0)
            both = dot(left, tiles_ref[pl.ds(t, 2)].reshape(2 * BLK, BLK), 1, 1)
            products += [both[:columns, :BLK], both[columns:, BLK:]]
        for u in range(unroll):
            acc_ref[meta_ref[0, step * unroll + u]] += products[u]

    bias = bias_ref[...]
    for b in range(row_blocks):
        out_ref[:, b * BLK : (b + 1) * BLK] = jnp.maximum(acc_ref[b] + bias, 0.0).astype(BF16)


def local(
    n_dom, n_feat,
    features, weight, out_bias, tile_values, tile_rows, tile_cols, tile_count, send_rows, hub_ids,
):
    rows, _ = features.shape
    cols = out_bias.shape[0]
    hubs = hub_ids.shape[0]
    slots, halo = send_rows.shape[1:]
    chunk = 8
    n_chunk = cols // chunk
    z_ring = n_dom // Y_RING
    blocks = (rows + slots * halo + hubs) // BLK
    vmem = pl.BlockSpec(memory_space=pltpu.VMEM)
    dma = pltpu.SemaphoreType.DMA
    tiles = tile_values.shape[0]
    shape = jax.ShapeDtypeStruct
    carried = 2 * blocks * cols * BLK + 2 * tile_values.size + 4 * (8 + cols) * BLK
    extended, held_tiles, meta, bias = pl.pallas_call(
        functools.partial(exchange_kernel, n_dom, n_feat, cols, chunk),
        out_shape=(
            pltpu.VMEM((blocks, cols, BLK), BF16),
            pltpu.VMEM(tile_values.shape, BF16),
            pltpu.SMEM((8, BLK), I32),
            pltpu.VMEM((cols, BLK), F32),
        ),
        in_specs=[pl.BlockSpec(memory_space=pltpu.HBM)] * 9,
        out_specs=(vmem, vmem, pl.BlockSpec(memory_space=pltpu.SMEM), vmem),
        scratch_shapes=[
            pltpu.VMEM((features.shape[1], rows), BF16),
            pltpu.VMEM(weight.shape, BF16),
            pltpu.VMEM((slots, halo), I32),
            pltpu.VMEM((hubs // BLK, BLK), I32),
            pltpu.VMEM((slots, LO, halo), BF16),
            pltpu.VMEM((Y_RING * HUB_MOST, hubs), BF16),
            pltpu.VMEM((n_feat, n_chunk, chunk, rows), BF16),
            pltpu.VMEM((n_chunk, n_feat - 1, chunk, rows), BF16),
            pltpu.VMEM((n_chunk, slots, halo // BLK, chunk, BLK), BF16),
            pltpu.VMEM((n_feat, cols // 2, BLK), BF16),
            pltpu.VMEM((n_feat - 1, cols // 2, BLK), BF16),
            pltpu.VMEM((cols // 2, BLK), BF16),
            pltpu.VMEM((Y_RING, cols // 2, BLK), BF16),
            pltpu.VMEM((cols, Y_RING * HUB_MOST), BF16),
            pltpu.VMEM((z_ring, cols, Y_RING * HUB_MOST), BF16),
            pltpu.VMEM((2, 1, tiles), I32),
            pltpu.VMEM((8, BLK), I32),
            pltpu.SMEM((1,), I32),
            pltpu.VMEM((1, cols), F32),
            dma((9,)),
            dma,
            dma((n_chunk,)),
            dma((slots,)),
            dma((slots,)),
            dma,
            dma,
            dma,
            dma,
            dma,
            dma,
            pltpu.SemaphoreType.REGULAR,
            pltpu.SemaphoreType.REGULAR,
            pltpu.SemaphoreType.REGULAR,
        ],
        compiler_params=pltpu.CompilerParams(
            collective_id=0,
            has_side_effects=True,
            vmem_limit_bytes=VMEM_MOST - carried - 65536,
        ),
        name="exchange",
    )(
        features.T, weight, send_rows[0], hub_ids.reshape(hubs // BLK, BLK), tile_values,
        tile_rows[None, :], tile_cols[None, :], tile_count, out_bias[None, :],
    )
    out_t = pl.pallas_call(
        tile_kernel,
        out_shape=shape((cols, rows), BF16),
        in_specs=[pl.BlockSpec(memory_space=pltpu.SMEM), vmem, vmem, vmem],
        out_specs=vmem,
        scratch_shapes=[pltpu.VMEM((rows // BLK + 1, cols, BLK), F32)],
        compiler_params=pltpu.CompilerParams(vmem_limit_bytes=16 * 2**20),
        name="tiles",
    )(meta, held_tiles, extended, bias)
    return out_t.T


def solution(mesh):
    in_specs = (
        P("dom", "feat"),
        P(),
        P("feat"),
        P("dom", None, None),
        P("dom"),
        P("dom"),
        P("dom"),
        P("dom", None, None),
        P(),
    )
    out_specs = P("dom", "feat")
    body = functools.partial(local, mesh.shape["dom"], mesh.shape["feat"])
    return jax.shard_map(body, mesh=mesh, in_specs=in_specs, out_specs=out_specs, check_vma=False)
```

```python
import functools

import jax
import jax.numpy as jnp
from jax import lax
from jax.experimental import pallas as pl
from jax.experimental.pallas import tpu as pltpu
from jax.sharding import PartitionSpec as P

REACH = 4
HUB_MOST = 48
Y_RING = 8
LO = 256
BLK = 128
OFFSETS = tuple(range(-REACH, 0)) + tuple(range(1, REACH + 1))
SEND_ORDER = (0, 7, 1, 6, 2, 5, 3, 4)
VMEM_MOST = 67_043_328
MESH = pl.DeviceIdType.MESH
F32, BF16, I32 = jnp.float32, jnp.bfloat16, jnp.int32


def dims(a, b):
    return (((a,), (b,)), ((), ()))


def dot(a, b, ca=1, cb=0):
    return lax.dot_general(a, b, dims(ca, cb), preferred_element_type=F32)


def ones_where(mask):
    return jnp.where(mask, 1.0, 0.0).astype(BF16)


def ascending(shape, swap=False):
    a, b = lax.broadcasted_iota(I32, shape, 0), lax.broadcasted_iota(I32, shape, 1)
    return b < a if swap else a < b


def pick_groups(stacked, group_of, groups, height):
    total = jnp.zeros((height, stacked.shape[1]), F32)
    for g in range(groups):
        total = jnp.where(group_of == g, stacked[g * height : (g + 1) * height], total)
    return total


def arrived_in(ref, sem):
    pltpu.make_async_copy(ref, ref, sem).wait()


def far_first(ring):
    return sorted(range(1, ring), key=lambda d: -min(d, ring - d))


def as_row(x):
    return jnp.concatenate([x[i : i + 1] for i in range(x.shape[0])], 1)


def exchange_kernel(
    n_dom, n_feat, cols, chunk,
    ft_hbm, w_hbm, send_hbm, hub_hbm, tiles_hbm, rows_hbm, cols_hbm, count_hbm, bias_hbm,
    ext_ref, tiles_ref, meta_smem, bias_ref,
    ft_ref, w_ref, send_ref, hub_ref, hot_ref, endhot_ref, sx, rx, sy,
    hx_out, hx, hub_out, hy, hpack, hz, meta_in, meta_ref, count_in, bias_in,
    in_sem, sxs, sxr, sys_, syr, hxs, hxr, hys, hyr, hzs, hzr, feat_in, near_in, ring_in,
):
    p = lax.axis_index("dom")
    j = lax.axis_index("feat")
    y = lax.rem(p, Y_RING)
    z = lax.div(p, Y_RING)
    z_ring = n_dom // Y_RING
    k_in, rows = ft_ref.shape
    n_chunk = cols // chunk
    his = rows // LO
    slots, halo = send_ref.shape
    own_blocks = rows // BLK
    slot_blocks = halo // BLK
    hub_first = own_blocks + slots * slot_blocks
    near_desk, ring_desk = n_feat - 1, n_feat - 3
    desks = (near_desk, ring_desk)
    at_desk = (j == near_desk) | (j == ring_desk)

    loads = []
    for i, (src, dst) in enumerate(
        (
            (hub_hbm, hub_ref), (ft_hbm, ft_ref), (w_hbm, w_ref), (send_hbm, send_ref),
            (rows_hbm, meta_in.at[0]), (cols_hbm, meta_in.at[1]),
            (count_hbm, count_in), (bias_hbm, bias_in), (tiles_hbm, tiles_ref),
        )
    ):
        loads.append(pltpu.make_async_copy(src, dst, in_sem.at[i]))
        loads[-1].start()

    def y_at(step):
        return z * Y_RING + lax.rem(y + step, Y_RING)

    def z_at(step):
        return lax.rem(z + step, z_ring) * Y_RING + y

    def feat_at(step):
        return lax.rem(j + step, n_feat)

    def tell(sem, dom, feat):
        pl.semaphore_signal(
            sem, inc=1, device_id={"dom": dom, "feat": feat}, device_id_type=MESH
        )

    def inside(o):
        return (p + o >= 0) & (p + o < n_dom)

    barrier = pltpu.get_barrier_semaphore()
    for other in range(n_feat):
        if other in desks:
            continue

        @pl.when(j != other)
        def _():
            tell(barrier, p, other)

    loads[0].wait()

    ids = hub_ref[...]
    hubs = ids.size
    mine = lax.div(ids, rows) == p
    mine_ones = ones_where(mine)
    side = ids.shape[0]
    in_row = dot(mine_ones, ones_where(ascending((BLK, BLK))))
    above = jnp.sum(dot(ones_where(ascending((side, side), True)), mine_ones), 1, keepdims=True)
    my_rank = (in_row + above).astype(I32)
    local_row = lax.rem(ids, rows)
    place = as_row(jnp.where(mine, lax.rem(my_rank + y * HUB_MOST, BLK), -1))
    taken = ones_where(lax.broadcasted_iota(I32, (BLK, hubs), 0) == place)
    halves = jnp.concatenate(
        [as_row(lax.rem(local_row, LO).astype(F32)), as_row((lax.div(local_row, LO) + 1).astype(F32))]
        + [jnp.zeros((14, hubs), F32)],
        0,
    ).astype(BF16)
    listed = dot(halves, taken, 1, 1)
    hub_row = (listed[0:1] + LO * (listed[1:2] - 1.0)).astype(I32)
    hub_pick = ones_where(lax.broadcasted_iota(I32, (rows, BLK), 0) == hub_row)

    f_in = w_ref.shape[0]
    loads[2].wait()
    pick = ones_where(
        lax.broadcasted_iota(I32, (BLK, f_in), 1)
        == lax.broadcasted_iota(I32, (BLK, f_in), 0) + j * k_in
    )
    w_mine = dot(pick, w_ref[...])
    w_t = w_mine.T.astype(BF16)[:, :k_in]

    loads[1].wait()
    ft = ft_ref[...]
    hub_ft = dot(ft, hub_pick).astype(BF16)
    hub_part = dot(w_t, hub_ft)
    half = cols // 2
    for d in range(n_feat):
        lower = hub_part[d * cols : d * cols + half]
        upper = hub_part[d * cols + half : (d + 1) * cols]
        hx_out[d] = (lower + pltpu.roll(upper, BLK // 2, 1)).astype(BF16)

    @pl.when(jnp.logical_not(at_desk))
    def _():
        pl.semaphore_wait(barrier, n_feat - 1)

    for desk in desks:

        @pl.when(j == desk - 1)
        def _():
            tell(feat_in, p, desk)

    @pl.when(at_desk)
    def _():
        pl.semaphore_wait(feat_in, 1)

    @pl.when(j == near_desk)
    def _():
        for o in OFFSETS:

            @pl.when(inside(o))
            def _():
                tell(barrier, p + o, near_desk)

        for d in range(1, Y_RING):
            tell(barrier, y_at(d), near_desk)

    @pl.when(j == ring_desk)
    def _():
        for d in range(1, z_ring):
            tell(barrier, z_at(d), ring_desk)

    for d in far_first(n_feat):
        copy = pltpu.make_async_remote_copy(
            src_ref=hx_out.at[feat_at(d)],
            dst_ref=hx.at[d - 1],
            send_sem=hxs,
            recv_sem=hxr,
            device_id={"feat": feat_at(d)},
            device_id_type=MESH,
        )
        copy.start()

    for h in range(n_chunk):
        left = jnp.concatenate(
            [w_t[d * cols + h * chunk : d * cols + (h + 1) * chunk] for d in range(n_feat)], 0
        )
        part = dot(left, ft).astype(BF16)
        for d in range(n_feat):
            sx[d, h] = part[d * chunk : (d + 1) * chunk]
        for d in far_first(n_feat):
            copy = pltpu.make_async_remote_copy(
                src_ref=sx.at[feat_at(d), h],
                dst_ref=rx.at[h, d - 1],
                send_sem=sxs,
                recv_sem=sxr.at[h],
                device_id={"feat": feat_at(d)},
                device_id_type=MESH,
            )
            copy.start()

    loads[3].wait()
    for s in range(slots):
        lo = lax.rem(send_ref[s : s + 1, :], LO)
        hot_ref[s] = ones_where(lax.broadcasted_iota(I32, (LO, halo), 0) == lo)
    packed = Y_RING * HUB_MOST
    ids_row = as_row(ids)
    owner = lax.div(ids_row, rows)
    owned = lax.broadcasted_iota(I32, (n_dom, hubs), 0) == owner
    earlier = dot(ones_where(owned), ones_where(ascending((hubs, hubs))))
    rank = jnp.sum(jnp.where(owned, earlier, 0.0), 0, keepdims=True).astype(I32)
    end_place = lax.rem(owner, Y_RING) * HUB_MOST + rank
    end_z = lax.div(owner, Y_RING)
    endhot_ref[...] = ones_where(lax.broadcasted_iota(I32, (packed, hubs), 0) == end_place)

    for i in range(4, 8):
        loads[i].wait()
    tiles = meta_in.shape[2]
    live = lax.broadcasted_iota(I32, (1, tiles), 1) < count_in[0]
    meta_ref[0:1, 0:tiles] = jnp.where(live, meta_in[0], own_blocks)
    meta_ref[1:2, 0:tiles] = meta_in[1]
    hand_over = pltpu.make_async_copy(meta_ref, meta_smem, in_sem.at[4])
    hand_over.start()
    eye = lax.broadcasted_iota(I32, (cols, cols), 0) == lax.broadcasted_iota(I32, (cols, cols), 1)
    bias = jnp.sum(jnp.where(eye, bias_in[...], 0.0), 1, keepdims=True)
    bias_ref[...] = jnp.broadcast_to(bias, (cols, BLK))

    for s in range(slots):

        @pl.when(jnp.logical_not(inside(-OFFSETS[s])))
        def _():
            first = own_blocks + s * slot_blocks
            ext_ref[first : first + slot_blocks] = jnp.zeros((slot_blocks, cols, BLK), BF16)

    @pl.when(j == near_desk)
    def _():
        before_p = lax.min(p, REACH)
        after_p = lax.min(n_dom - 1 - p, REACH)
        pl.semaphore_wait(barrier, before_p + after_p + Y_RING - 1)
        for other in range(n_feat - 1):
            tell(near_in, p, other)

    arrived_in(hx, hxr)
    hub_sum = hx_out[j].astype(F32)
    for d in range(1, n_feat):
        hub_sum = hub_sum + hx[d - 1].astype(F32)
    hub_mine = hub_sum.astype(BF16)
    hub_out[...] = hub_mine
    hy[y] = hub_mine

    @pl.when(j != near_desk)
    def _():
        pl.semaphore_wait(near_in, 1)

    for d in far_first(Y_RING):
        copy = pltpu.make_async_remote_copy(
            src_ref=hub_out,
            dst_ref=hy.at[y],
            send_sem=hys,
            recv_sem=hyr,
            device_id={"dom": y_at(d)},
            device_id_type=MESH,
        )
        copy.start()

    def bulk(h):
        span = slice(h * chunk, (h + 1) * chunk)
        arrived_in(rx.at[h], sxr.at[h])
        total = sx[j, h].astype(F32)
        for d in range(1, n_feat):
            total = total + rx[h, d - 1].astype(F32)
        proj = total.astype(BF16)
        for b in range(own_blocks):
            ext_ref[b, span, :] = proj[:, b * BLK : (b + 1) * BLK]
        stacked = jnp.concatenate([proj[:, g * LO : (g + 1) * LO] for g in range(his)], 0)
        for s in SEND_ORDER:
            hi = lax.div(send_ref[s : s + 1, :], LO)
            rows_out = pick_groups(dot(stacked, hot_ref[s]), hi, his, chunk).astype(BF16)
            for b in range(slot_blocks):
                sy[h, s, b] = rows_out[:, b * BLK : (b + 1) * BLK]
            first = own_blocks + s * slot_blocks
            copy = pltpu.make_async_remote_copy(
                src_ref=sy.at[h, s],
                dst_ref=ext_ref.at[first : first + slot_blocks, span, :],
                send_sem=sys_.at[s],
                recv_sem=syr.at[s],
                device_id={"dom": p + OFFSETS[s]},
                device_id_type=MESH,
            )

            @pl.when(inside(OFFSETS[s]))
            def _():
                copy.start()

    bulk(0)

    @pl.when(j == ring_desk)
    def _():
        pl.semaphore_wait(barrier, z_ring - 1)
        for other in range(n_feat):
            if other != ring_desk:
                tell(ring_in, p, other)

    bulk(1)

    arrived_in(hy.at[0 : Y_RING - 1], hyr)
    arrived = [hy[source].astype(F32) for source in range(Y_RING)]
    for t in range(packed // BLK):
        lane = lax.broadcasted_iota(I32, (half, BLK), 1) + t * BLK
        low_tile = jnp.zeros((half, BLK), F32)
        high_tile = jnp.zeros((half, BLK), F32)
        for source in range(Y_RING):
            low, high = source * HUB_MOST, (source + 1) * HUB_MOST
            if high <= t * BLK or low >= (t + 1) * BLK:
                continue
            here = (lane >= low) & (lane < high)
            low_tile = jnp.where(here, arrived[source], low_tile)
            high_tile = jnp.where(here, pltpu.roll(arrived[source], BLK // 2, 1), high_tile)
        hpack[:half, t * BLK : (t + 1) * BLK] = low_tile.astype(BF16)
        hpack[half:, t * BLK : (t + 1) * BLK] = high_tile.astype(BF16)
    hz[z] = hpack[...]

    @pl.when(j != ring_desk)
    def _():
        pl.semaphore_wait(ring_in, 1)

    for d in far_first(z_ring):
        copy = pltpu.make_async_remote_copy(
            src_ref=hpack,
            dst_ref=hz.at[z],
            send_sem=hzs,
            recv_sem=hzr,
            device_id={"dom": z_at(d)},
            device_id_type=MESH,
        )
        copy.start()

    for h in range(2, n_chunk):
        bulk(h)

    arrived_in(hz.at[0 : z_ring - 1], hzr)
    everyone = jnp.concatenate([hz[source] for source in range(z_ring)], 0)
    hub_block = pick_groups(dot(everyone, endhot_ref[...]), end_z, z_ring, cols).astype(BF16)
    for b in range(hubs // BLK):
        ext_ref[hub_first + b] = hub_block[:, b * BLK : (b + 1) * BLK]

    loads[8].wait()
    hand_over.wait()
    for s in range(slots):
        first = own_blocks + s * slot_blocks
        slot_rows = ext_ref.at[first : first + slot_blocks]

        @pl.when(inside(-OFFSETS[s]))
        def _():
            arrived_in(slot_rows, syr.at[s])

        @pl.when(inside(OFFSETS[s]))
        def _():
            arrived_in(slot_rows, sys_.at[s])

    arrived_in(hx, hxs)
    arrived_in(rx, sxs)
    arrived_in(hy.at[0 : Y_RING - 1], hys)
    arrived_in(hz.at[0 : z_ring - 1], hzs)


def tile_kernel(meta_ref, tiles_ref, ext_ref, bias_ref, out_ref, acc_ref):
    row_blocks = acc_ref.shape[0] - 1
    acc_ref[...] = jnp.zeros_like(acc_ref)
    unroll = 36
    columns = ext_ref.shape[1]

    @pl.loop(0, tiles_ref.shape[0] // unroll)
    def _(step):
        products = []
        for u in range(0, unroll, 2):
            t = step * unroll + u
            left = jnp.concatenate([ext_ref[meta_ref[1, t]], ext_ref[meta_ref[1, t + 1]]], 0)
            both = dot(left, tiles_ref[pl.ds(t, 2)].reshape(2 * BLK, BLK), 1, 1)
            products += [both[:columns, :BLK], both[columns:, BLK:]]
        for u in range(unroll):
            acc_ref[meta_ref[0, step * unroll + u]] += products[u]

    bias = bias_ref[...]
    for b in range(row_blocks):
        out_ref[:, b * BLK : (b + 1) * BLK] = jnp.maximum(acc_ref[b] + bias, 0.0).astype(BF16)


def local(
    n_dom, n_feat,
    features, weight, out_bias, tile_values, tile_rows, tile_cols, tile_count, send_rows, hub_ids,
):
    rows, _ = features.shape
    cols = out_bias.shape[0]
    hubs = hub_ids.shape[0]
    slots, halo = send_rows.shape[1:]
    chunk = 8
    n_chunk = cols // chunk
    z_ring = n_dom // Y_RING
    blocks = (rows + slots * halo + hubs) // BLK
    vmem = pl.BlockSpec(memory_space=pltpu.VMEM)
    dma = pltpu.SemaphoreType.DMA
    tiles = tile_values.shape[0]
    shape = jax.ShapeDtypeStruct
    carried = 2 * blocks * cols * BLK + 2 * tile_values.size + 4 * (8 + cols) * BLK
    extended, held_tiles, meta, bias = pl.pallas_call(
        functools.partial(exchange_kernel, n_dom, n_feat, cols, chunk),
        out_shape=(
            pltpu.VMEM((blocks, cols, BLK), BF16),
            pltpu.VMEM(tile_values.shape, BF16),
            pltpu.SMEM((8, BLK), I32),
            pltpu.VMEM((cols, BLK), F32),
        ),
        in_specs=[pl.BlockSpec(memory_space=pltpu.HBM)] * 9,
        out_specs=(vmem, vmem, pl.BlockSpec(memory_space=pltpu.SMEM), vmem),
        scratch_shapes=[
            pltpu.VMEM((features.shape[1], rows), BF16),
            pltpu.VMEM(weight.shape, BF16),
            pltpu.VMEM((slots, halo), I32),
            pltpu.VMEM((hubs // BLK, BLK), I32),
            pltpu.VMEM((slots, LO, halo), BF16),
            pltpu.VMEM((Y_RING * HUB_MOST, hubs), BF16),
            pltpu.VMEM((n_feat, n_chunk, chunk, rows), BF16),
            pltpu.VMEM((n_chunk, n_feat - 1, chunk, rows), BF16),
            pltpu.VMEM((n_chunk, slots, halo // BLK, chunk, BLK), BF16),
            pltpu.VMEM((n_feat, cols // 2, BLK), BF16),
            pltpu.VMEM((n_feat - 1, cols // 2, BLK), BF16),
            pltpu.VMEM((cols // 2, BLK), BF16),
            pltpu.VMEM((Y_RING, cols // 2, BLK), BF16),
            pltpu.VMEM((cols, Y_RING * HUB_MOST), BF16),
            pltpu.VMEM((z_ring, cols, Y_RING * HUB_MOST), BF16),
            pltpu.VMEM((2, 1, tiles), I32),
            pltpu.VMEM((8, BLK), I32),
            pltpu.SMEM((1,), I32),
            pltpu.VMEM((1, cols), F32),
            dma((9,)),
            dma,
            dma((n_chunk,)),
            dma((slots,)),
            dma((slots,)),
            dma,
            dma,
            dma,
            dma,
            dma,
            dma,
            pltpu.SemaphoreType.REGULAR,
            pltpu.SemaphoreType.REGULAR,
            pltpu.SemaphoreType.REGULAR,
        ],
        compiler_params=pltpu.CompilerParams(
            collective_id=0,
            has_side_effects=True,
            vmem_limit_bytes=VMEM_MOST - carried - 65536,
        ),
        name="exchange",
    )(
        features.T, weight, send_rows[0], hub_ids.reshape(hubs // BLK, BLK), tile_values,
        tile_rows[None, :], tile_cols[None, :], tile_count, out_bias[None, :],
    )
    out_t = pl.pallas_call(
        tile_kernel,
        out_shape=shape((cols, rows), BF16),
        in_specs=[pl.BlockSpec(memory_space=pltpu.SMEM), vmem, vmem, vmem],
        out_specs=vmem,
        scratch_shapes=[pltpu.VMEM((rows // BLK + 1, cols, BLK), F32)],
        compiler_params=pltpu.CompilerParams(vmem_limit_bytes=16 * 2**20),
        name="tiles",
    )(meta, held_tiles, extended, bias)
    return out_t.T


def solution(mesh):
    in_specs = (
        P("dom", "feat"),
        P(),
        P("feat"),
        P("dom", None, None),
        P("dom"),
        P("dom"),
        P("dom"),
        P("dom", None, None),
        P(),
    )
    out_specs = P("dom", "feat")
    body = functools.partial(local, mesh.shape["dom"], mesh.shape["feat"])
    return jax.shard_map(body, mesh=mesh, in_specs=in_specs, out_specs=out_specs, check_vma=False)
```

```python
import functools

import jax
import jax.numpy as jnp
from jax import lax
from jax.experimental import pallas as pl
from jax.experimental.pallas import tpu as pltpu
from jax.sharding import PartitionSpec as P

REACH = 4
HUB_MOST = 48
Y_RING = 8
LO = 256
BLK = 128
OFFSETS = tuple(range(-REACH, 0)) + tuple(range(1, REACH + 1))
SEND_ORDER = (0, 7, 1, 6, 2, 5, 3, 4)
VMEM_MOST = 67_043_328
MESH = pl.DeviceIdType.MESH
F32, BF16, I32 = jnp.float32, jnp.bfloat16, jnp.int32


def dims(a, b):
    return (((a,), (b,)), ((), ()))


def dot(a, b, ca=1, cb=0):
    return lax.dot_general(a, b, dims(ca, cb), preferred_element_type=F32)


def ones_where(mask):
    return jnp.where(mask, 1.0, 0.0).astype(BF16)


def ascending(shape, swap=False):
    a, b = lax.broadcasted_iota(I32, shape, 0), lax.broadcasted_iota(I32, shape, 1)
    return b < a if swap else a < b


def pick_groups(stacked, group_of, groups, height):
    total = jnp.zeros((height, stacked.shape[1]), F32)
    for g in range(groups):
        total = jnp.where(group_of == g, stacked[g * height : (g + 1) * height], total)
    return total


def arrived_in(ref, sem):
    pltpu.make_async_copy(ref, ref, sem).wait()


def far_first(ring):
    return sorted(range(1, ring), key=lambda d: -min(d, ring - d))


def as_row(x):
    return jnp.concatenate([x[i : i + 1] for i in range(x.shape[0])], 1)


def exchange_kernel(
    n_dom, n_feat, cols, chunk,
    ft_hbm, w_hbm, send_hbm, hub_hbm, tiles_hbm, rows_hbm, cols_hbm, count_hbm, bias_hbm,
    ext_ref, tiles_ref, meta_smem, bias_ref,
    ft_ref, w_ref, send_ref, hub_ref, hot_ref, endhot_ref, sx, rx, sy,
    hx_out, hx, hub_out, hy, hpack, hz, meta_in, meta_ref, count_in, bias_in,
    in_sem, sxs, sxr, sys_, syr, hxs, hxr, hys, hyr, hzs, hzr, feat_in, near_in, ring_in,
):
    p = lax.axis_index("dom")
    j = lax.axis_index("feat")
    y = lax.rem(p, Y_RING)
    z = lax.div(p, Y_RING)
    z_ring = n_dom // Y_RING
    k_in, rows = ft_ref.shape
    n_chunk = cols // chunk
    his = rows // LO
    slots, halo = send_ref.shape
    own_blocks = rows // BLK
    slot_blocks = halo // BLK
    hub_first = own_blocks + slots * slot_blocks
    near_desk, ring_desk = n_feat - 1, n_feat - 3
    desks = (near_desk, ring_desk)
    at_desk = (j == near_desk) | (j == ring_desk)

    loads = []
    for i, (src, dst) in enumerate(
        (
            (hub_hbm, hub_ref), (ft_hbm, ft_ref), (w_hbm, w_ref), (send_hbm, send_ref),
            (rows_hbm, meta_in.at[0]), (cols_hbm, meta_in.at[1]),
            (count_hbm, count_in), (bias_hbm, bias_in), (tiles_hbm, tiles_ref),
        )
    ):
        loads.append(pltpu.make_async_copy(src, dst, in_sem.at[i]))
        loads[-1].start()

    def y_at(step):
        return z * Y_RING + lax.rem(y + step, Y_RING)

    def z_at(step):
        return lax.rem(z + step, z_ring) * Y_RING + y

    def feat_at(step):
        return lax.rem(j + step, n_feat)

    def tell(sem, dom, feat):
        pl.semaphore_signal(
            sem, inc=1, device_id={"dom": dom, "feat": feat}, device_id_type=MESH
        )

    def inside(o):
        return (p + o >= 0) & (p + o < n_dom)

    barrier = pltpu.get_barrier_semaphore()
    for other in range(n_feat):
        if other in desks:
            continue

        @pl.when(j != other)
        def _():
            tell(barrier, p, other)

    loads[0].wait()

    ids = hub_ref[...]
    hubs = ids.size
    mine = lax.div(ids, rows) == p
    mine_ones = ones_where(mine)
    side = ids.shape[0]
    in_row = dot(mine_ones, ones_where(ascending((BLK, BLK))))
    above = jnp.sum(dot(ones_where(ascending((side, side), True)), mine_ones), 1, keepdims=True)
    my_rank = (in_row + above).astype(I32)
    local_row = lax.rem(ids, rows)
    place = as_row(jnp.where(mine, lax.rem(my_rank + y * HUB_MOST, BLK), -1))
    taken = ones_where(lax.broadcasted_iota(I32, (BLK, hubs), 0) == place)
    halves = jnp.concatenate(
        [as_row(lax.rem(local_row, LO).astype(F32)), as_row((lax.div(local_row, LO) + 1).astype(F32))]
        + [jnp.zeros((14, hubs), F32)],
        0,
    ).astype(BF16)
    listed = dot(halves, taken, 1, 1)
    hub_row = (listed[0:1] + LO * (listed[1:2] - 1.0)).astype(I32)
    hub_pick = ones_where(lax.broadcasted_iota(I32, (rows, BLK), 0) == hub_row)

    f_in = w_ref.shape[0]
    loads[2].wait()
    pick = ones_where(
        lax.broadcasted_iota(I32, (BLK, f_in), 1)
        == lax.broadcasted_iota(I32, (BLK, f_in), 0) + j * k_in
    )
    w_mine = dot(pick, w_ref[...])
    w_t = w_mine.T.astype(BF16)[:, :k_in]

    loads[1].wait()
    ft = ft_ref[...]
    hub_ft = dot(ft, hub_pick).astype(BF16)
    hub_part = dot(w_t, hub_ft)
    half = cols // 2
    for d in range(n_feat):
        lower = hub_part[d * cols : d * cols + half]
        upper = hub_part[d * cols + half : (d + 1) * cols]
        hx_out[d] = (lower + pltpu.roll(upper, BLK // 2, 1)).astype(BF16)

    @pl.when(jnp.logical_not(at_desk))
    def _():
        pl.semaphore_wait(barrier, n_feat - 1)

    for desk in desks:

        @pl.when(j == desk - 1)
        def _():
            tell(feat_in, p, desk)

    @pl.when(at_desk)
    def _():
        pl.semaphore_wait(feat_in, 1)

    @pl.when(j == near_desk)
    def _():
        for o in OFFSETS:

            @pl.when(inside(o))
            def _():
                tell(barrier, p + o, near_desk)

        for d in range(1, Y_RING):
            tell(barrier, y_at(d), near_desk)

    @pl.when(j == ring_desk)
    def _():
        for d in range(1, z_ring):
            tell(barrier, z_at(d), ring_desk)

    for d in far_first(n_feat):
        copy = pltpu.make_async_remote_copy(
            src_ref=hx_out.at[feat_at(d)],
            dst_ref=hx.at[d - 1],
            send_sem=hxs,
            recv_sem=hxr,
            device_id={"feat": feat_at(d)},
            device_id_type=MESH,
        )
        copy.start()

    for h in range(n_chunk):
        left = jnp.concatenate(
            [w_t[d * cols + h * chunk : d * cols + (h + 1) * chunk] for d in range(n_feat)], 0
        )
        part = dot(left, ft).astype(BF16)
        for d in range(n_feat):
            sx[d, h] = part[d * chunk : (d + 1) * chunk]
        for d in far_first(n_feat):
            copy = pltpu.make_async_remote_copy(
                src_ref=sx.at[feat_at(d), h],
                dst_ref=rx.at[h, d - 1],
                send_sem=sxs,
                recv_sem=sxr.at[h],
                device_id={"feat": feat_at(d)},
                device_id_type=MESH,
            )
            copy.start()

    loads[3].wait()
    for s in range(slots):
        lo = lax.rem(send_ref[s : s + 1, :], LO)
        hot_ref[s] = ones_where(lax.broadcasted_iota(I32, (LO, halo), 0) == lo)
    @pl.when(j == near_desk)
    def _():
        before_p = lax.min(p, REACH)
        after_p = lax.min(n_dom - 1 - p, REACH)
        pl.semaphore_wait(barrier, before_p + after_p + Y_RING - 1)
        for other in range(n_feat - 1):
            tell(near_in, p, other)

    arrived_in(hx, hxr)
    hub_sum = hx_out[j].astype(F32)
    for d in range(1, n_feat):
        hub_sum = hub_sum + hx[d - 1].astype(F32)
    hub_mine = hub_sum.astype(BF16)
    hub_out[...] = hub_mine
    hy[y] = hub_mine

    @pl.when(j != near_desk)
    def _():
        pl.semaphore_wait(near_in, 1)

    for d in far_first(Y_RING):
        copy = pltpu.make_async_remote_copy(
            src_ref=hub_out,
            dst_ref=hy.at[y],
            send_sem=hys,
            recv_sem=hyr,
            device_id={"dom": y_at(d)},
            device_id_type=MESH,
        )
        copy.start()

    packed = Y_RING * HUB_MOST

    def bulk(h):
        span = slice(h * chunk, (h + 1) * chunk)
        arrived_in(rx.at[h], sxr.at[h])
        total = sx[j, h].astype(F32)
        for d in range(1, n_feat):
            total = total + rx[h, d - 1].astype(F32)
        proj = total.astype(BF16)
        for b in range(own_blocks):
            ext_ref[b, span, :] = proj[:, b * BLK : (b + 1) * BLK]
        stacked = jnp.concatenate([proj[:, g * LO : (g + 1) * LO] for g in range(his)], 0)
        for s in SEND_ORDER:
            hi = lax.div(send_ref[s : s + 1, :], LO)
            rows_out = pick_groups(dot(stacked, hot_ref[s]), hi, his, chunk).astype(BF16)
            for b in range(slot_blocks):
                sy[h, s, b] = rows_out[:, b * BLK : (b + 1) * BLK]
            first = own_blocks + s * slot_blocks
            copy = pltpu.make_async_remote_copy(
                src_ref=sy.at[h, s],
                dst_ref=ext_ref.at[first : first + slot_blocks, span, :],
                send_sem=sys_.at[s],
                recv_sem=syr.at[s],
                device_id={"dom": p + OFFSETS[s]},
                device_id_type=MESH,
            )

            @pl.when(inside(OFFSETS[s]))
            def _():
                copy.start()

    bulk(0)

    @pl.when(j == ring_desk)
    def _():
        pl.semaphore_wait(barrier, z_ring - 1)
        for other in range(n_feat):
            if other != ring_desk:
                tell(ring_in, p, other)

    bulk(1)

    arrived_in(hy.at[0 : Y_RING - 1], hyr)
    arrived = [hy[source].astype(F32) for source in range(Y_RING)]
    for t in range(packed // BLK):
        lane = lax.broadcasted_iota(I32, (half, BLK), 1) + t * BLK
        low_tile = jnp.zeros((half, BLK), F32)
        high_tile = jnp.zeros((half, BLK), F32)
        for source in range(Y_RING):
            low, high = source * HUB_MOST, (source + 1) * HUB_MOST
            if high <= t * BLK or low >= (t + 1) * BLK:
                continue
            here = (lane >= low) & (lane < high)
            low_tile = jnp.where(here, arrived[source], low_tile)
            high_tile = jnp.where(here, pltpu.roll(arrived[source], BLK // 2, 1), high_tile)
        hpack[:half, t * BLK : (t + 1) * BLK] = low_tile.astype(BF16)
        hpack[half:, t * BLK : (t + 1) * BLK] = high_tile.astype(BF16)
    hz[z] = hpack[...]

    @pl.when(j != ring_desk)
    def _():
        pl.semaphore_wait(ring_in, 1)

    for d in far_first(z_ring):
        copy = pltpu.make_async_remote_copy(
            src_ref=hpack,
            dst_ref=hz.at[z],
            send_sem=hzs,
            recv_sem=hzr,
            device_id={"dom": z_at(d)},
            device_id_type=MESH,
        )
        copy.start()

    for h in range(2, n_chunk):
        bulk(h)

    ids_row = as_row(ids)
    owner = lax.div(ids_row, rows)
    owned = lax.broadcasted_iota(I32, (n_dom, hubs), 0) == owner
    earlier = dot(ones_where(owned), ones_where(ascending((hubs, hubs))))
    rank = jnp.sum(jnp.where(owned, earlier, 0.0), 0, keepdims=True).astype(I32)
    end_place = lax.rem(owner, Y_RING) * HUB_MOST + rank
    end_z = lax.div(owner, Y_RING)
    endhot_ref[...] = ones_where(lax.broadcasted_iota(I32, (packed, hubs), 0) == end_place)

    for i in range(4, 8):
        loads[i].wait()
    tiles = meta_in.shape[2]
    live = lax.broadcasted_iota(I32, (1, tiles), 1) < count_in[0]
    meta_ref[0:1, 0:tiles] = jnp.where(live, meta_in[0], own_blocks)
    meta_ref[1:2, 0:tiles] = meta_in[1]
    hand_over = pltpu.make_async_copy(meta_ref, meta_smem, in_sem.at[4])
    hand_over.start()
    eye = lax.broadcasted_iota(I32, (cols, cols), 0) == lax.broadcasted_iota(I32, (cols, cols), 1)
    bias = jnp.sum(jnp.where(eye, bias_in[...], 0.0), 1, keepdims=True)
    bias_ref[...] = jnp.broadcast_to(bias, (cols, BLK))

    for s in range(slots):

        @pl.when(jnp.logical_not(inside(-OFFSETS[s])))
        def _():
            first = own_blocks + s * slot_blocks
            ext_ref[first : first + slot_blocks] = jnp.zeros((slot_blocks, cols, BLK), BF16)

    arrived_in(hz.at[0 : z_ring - 1], hzr)
    everyone = jnp.concatenate([hz[source] for source in range(z_ring)], 0)
    hub_block = pick_groups(dot(everyone, endhot_ref[...]), end_z, z_ring, cols).astype(BF16)
    for b in range(hubs // BLK):
        ext_ref[hub_first + b] = hub_block[:, b * BLK : (b + 1) * BLK]

    loads[8].wait()
    hand_over.wait()
    for s in range(slots):
        first = own_blocks + s * slot_blocks
        slot_rows = ext_ref.at[first : first + slot_blocks]

        @pl.when(inside(-OFFSETS[s]))
        def _():
            arrived_in(slot_rows, syr.at[s])

        @pl.when(inside(OFFSETS[s]))
        def _():
            arrived_in(slot_rows, sys_.at[s])

    arrived_in(hx, hxs)
    arrived_in(rx, sxs)
    arrived_in(hy.at[0 : Y_RING - 1], hys)
    arrived_in(hz.at[0 : z_ring - 1], hzs)


def tile_kernel(meta_ref, tiles_ref, ext_ref, bias_ref, out_ref, acc_ref):
    row_blocks = acc_ref.shape[0] - 1
    acc_ref[...] = jnp.zeros_like(acc_ref)
    unroll = tiles_ref.shape[0]
    columns = ext_ref.shape[1]

    @pl.loop(0, tiles_ref.shape[0] // unroll)
    def _(step):
        products = []
        for u in range(0, unroll, 2):
            t = step * unroll + u
            left = jnp.concatenate([ext_ref[meta_ref[1, t]], ext_ref[meta_ref[1, t + 1]]], 0)
            both = dot(left, tiles_ref[pl.ds(t, 2)].reshape(2 * BLK, BLK), 1, 1)
            products += [both[:columns, :BLK], both[columns:, BLK:]]
        for u in range(unroll):
            acc_ref[meta_ref[0, step * unroll + u]] += products[u]

    bias = bias_ref[...]
    for b in range(row_blocks):
        out_ref[:, b * BLK : (b + 1) * BLK] = jnp.maximum(acc_ref[b] + bias, 0.0).astype(BF16)


def local(
    n_dom, n_feat,
    features, weight, out_bias, tile_values, tile_rows, tile_cols, tile_count, send_rows, hub_ids,
):
    rows, _ = features.shape
    cols = out_bias.shape[0]
    hubs = hub_ids.shape[0]
    slots, halo = send_rows.shape[1:]
    chunk = 8
    n_chunk = cols // chunk
    z_ring = n_dom // Y_RING
    blocks = (rows + slots * halo + hubs) // BLK
    vmem = pl.BlockSpec(memory_space=pltpu.VMEM)
    dma = pltpu.SemaphoreType.DMA
    tiles = tile_values.shape[0]
    shape = jax.ShapeDtypeStruct
    carried = 2 * blocks * cols * BLK + 2 * tile_values.size + 4 * (8 + cols) * BLK
    extended, held_tiles, meta, bias = pl.pallas_call(
        functools.partial(exchange_kernel, n_dom, n_feat, cols, chunk),
        out_shape=(
            pltpu.VMEM((blocks, cols, BLK), BF16),
            pltpu.VMEM(tile_values.shape, BF16),
            pltpu.SMEM((8, BLK), I32),
            pltpu.VMEM((cols, BLK), F32),
        ),
        in_specs=[pl.BlockSpec(memory_space=pltpu.HBM)] * 9,
        out_specs=(vmem, vmem, pl.BlockSpec(memory_space=pltpu.SMEM), vmem),
        scratch_shapes=[
            pltpu.VMEM((features.shape[1], rows), BF16),
            pltpu.VMEM(weight.shape, BF16),
            pltpu.VMEM((slots, halo), I32),
            pltpu.VMEM((hubs // BLK, BLK), I32),
            pltpu.VMEM((slots, LO, halo), BF16),
            pltpu.VMEM((Y_RING * HUB_MOST, hubs), BF16),
            pltpu.VMEM((n_feat, n_chunk, chunk, rows), BF16),
            pltpu.VMEM((n_chunk, n_feat - 1, chunk, rows), BF16),
            pltpu.VMEM((n_chunk, slots, halo // BLK, chunk, BLK), BF16),
            pltpu.VMEM((n_feat, cols // 2, BLK), BF16),
            pltpu.VMEM((n_feat - 1, cols // 2, BLK), BF16),
            pltpu.VMEM((cols // 2, BLK), BF16),
            pltpu.VMEM((Y_RING, cols // 2, BLK), BF16),
            pltpu.VMEM((cols, Y_RING * HUB_MOST), BF16),
            pltpu.VMEM((z_ring, cols, Y_RING * HUB_MOST), BF16),
            pltpu.VMEM((2, 1, tiles), I32),
            pltpu.VMEM((8, BLK), I32),
            pltpu.SMEM((1,), I32),
            pltpu.VMEM((1, cols), F32),
            dma((9,)),
            dma,
            dma((n_chunk,)),
            dma((slots,)),
            dma((slots,)),
            dma,
            dma,
            dma,
            dma,
            dma,
            dma,
            pltpu.SemaphoreType.REGULAR,
            pltpu.SemaphoreType.REGULAR,
            pltpu.SemaphoreType.REGULAR,
        ],
        compiler_params=pltpu.CompilerParams(
            collective_id=0,
            has_side_effects=True,
            vmem_limit_bytes=VMEM_MOST - carried - 65536,
        ),
        name="exchange",
    )(
        features.T, weight, send_rows[0], hub_ids.reshape(hubs // BLK, BLK), tile_values,
        tile_rows[None, :], tile_cols[None, :], tile_count, out_bias[None, :],
    )
    out_t = pl.pallas_call(
        tile_kernel,
        out_shape=shape((cols, rows), BF16),
        in_specs=[pl.BlockSpec(memory_space=pltpu.SMEM), vmem, vmem, vmem],
        out_specs=vmem,
        scratch_shapes=[pltpu.VMEM((rows // BLK + 1, cols, BLK), F32)],
        compiler_params=pltpu.CompilerParams(vmem_limit_bytes=16 * 2**20),
        name="tiles",
    )(meta, held_tiles, extended, bias)
    return out_t.T


def solution(mesh):
    in_specs = (
        P("dom", "feat"),
        P(),
        P("feat"),
        P("dom", None, None),
        P("dom"),
        P("dom"),
        P("dom"),
        P("dom", None, None),
        P(),
    )
    out_specs = P("dom", "feat")
    body = functools.partial(local, mesh.shape["dom"], mesh.shape["feat"])
    return jax.shard_map(body, mesh=mesh, in_specs=in_specs, out_specs=out_specs, check_vma=False)
```

```python
import functools

import jax
import jax.numpy as jnp
from jax import lax
from jax.experimental import pallas as pl
from jax.experimental.pallas import tpu as pltpu
from jax.sharding import PartitionSpec as P

REACH = 4
HUB_MOST = 48
Y_RING = 8
LO = 256
BLK = 128
OFFSETS = tuple(range(-REACH, 0)) + tuple(range(1, REACH + 1))
SEND_ORDER = (0, 7, 1, 6, 2, 5, 3, 4)
VMEM_MOST = 67_043_328
MESH = pl.DeviceIdType.MESH
F32, BF16, I32 = jnp.float32, jnp.bfloat16, jnp.int32


def dims(a, b):
    return (((a,), (b,)), ((), ()))


def dot(a, b, ca=1, cb=0):
    return lax.dot_general(a, b, dims(ca, cb), preferred_element_type=F32)


def ones_where(mask):
    return jnp.where(mask, 1.0, 0.0).astype(BF16)


def ascending(shape, swap=False):
    a, b = lax.broadcasted_iota(I32, shape, 0), lax.broadcasted_iota(I32, shape, 1)
    return b < a if swap else a < b


def pick_groups(stacked, group_of, groups, height):
    total = jnp.zeros((height, stacked.shape[1]), F32)
    for g in range(groups):
        total = jnp.where(group_of == g, stacked[g * height : (g + 1) * height], total)
    return total


def arrived_in(ref, sem):
    pltpu.make_async_copy(ref, ref, sem).wait()


def far_first(ring):
    return sorted(range(1, ring), key=lambda d: -min(d, ring - d))


def as_row(x):
    return jnp.concatenate([x[i : i + 1] for i in range(x.shape[0])], 1)


def exchange_kernel(
    n_dom, n_feat, cols, chunk,
    ft_hbm, w_hbm, send_hbm, hub_hbm, tiles_hbm, rows_hbm, cols_hbm, count_hbm, bias_hbm,
    ext_ref, tiles_ref, meta_smem, bias_ref,
    ft_ref, w_ref, send_ref, hub_ref, hot_ref, endhot_ref, sx, rx, sy,
    hx_out, hx, hub_out, hy, hpack, hz, meta_in, meta_ref, count_in, bias_in,
    in_sem, sxs, sxr, sys_, syr, hxs, hxr, hys, hyr, hzs, hzr, feat_in, near_in, ring_in,
):
    p = lax.axis_index("dom")
    j = lax.axis_index("feat")
    y = lax.rem(p, Y_RING)
    z = lax.div(p, Y_RING)
    z_ring = n_dom // Y_RING
    k_in, rows = ft_ref.shape
    n_chunk = cols // chunk
    his = rows // LO
    slots, halo = send_ref.shape
    own_blocks = rows // BLK
    slot_blocks = halo // BLK
    hub_first = own_blocks + slots * slot_blocks
    near_desk, ring_desk = n_feat - 1, n_feat - 3
    desks = (near_desk, ring_desk)
    at_desk = (j == near_desk) | (j == ring_desk)

    loads = []
    for i, (src, dst) in enumerate(
        (
            (hub_hbm, hub_ref), (ft_hbm, ft_ref), (w_hbm, w_ref), (send_hbm, send_ref),
            (rows_hbm, meta_in.at[0]), (cols_hbm, meta_in.at[1]),
            (count_hbm, count_in), (bias_hbm, bias_in), (tiles_hbm, tiles_ref),
        )
    ):
        loads.append(pltpu.make_async_copy(src, dst, in_sem.at[i]))
        loads[-1].start()

    def y_at(step):
        return z * Y_RING + lax.rem(y + step, Y_RING)

    def z_at(step):
        return lax.rem(z + step, z_ring) * Y_RING + y

    def feat_at(step):
        return lax.rem(j + step, n_feat)

    def tell(sem, dom, feat):
        pl.semaphore_signal(
            sem, inc=1, device_id={"dom": dom, "feat": feat}, device_id_type=MESH
        )

    def inside(o):
        return (p + o >= 0) & (p + o < n_dom)

    barrier = pltpu.get_barrier_semaphore()
    for other in range(n_feat):
        if other in desks:
            continue

        @pl.when(j != other)
        def _():
            tell(barrier, p, other)

    loads[0].wait()

    ids = hub_ref[...]
    hubs = ids.size
    mine = lax.div(ids, rows) == p
    mine_ones = ones_where(mine)
    side = ids.shape[0]
    in_row = dot(mine_ones, ones_where(ascending((BLK, BLK))))
    above = jnp.sum(dot(ones_where(ascending((side, side), True)), mine_ones), 1, keepdims=True)
    my_rank = (in_row + above).astype(I32)
    local_row = lax.rem(ids, rows)
    place = as_row(jnp.where(mine, lax.rem(my_rank + y * HUB_MOST, BLK), -1))
    taken = ones_where(lax.broadcasted_iota(I32, (BLK, hubs), 0) == place)
    halves = jnp.concatenate(
        [as_row(lax.rem(local_row, LO).astype(F32)), as_row((lax.div(local_row, LO) + 1).astype(F32))]
        + [jnp.zeros((14, hubs), F32)],
        0,
    ).astype(BF16)
    listed = dot(halves, taken, 1, 1)
    hub_row = (listed[0:1] + LO * (listed[1:2] - 1.0)).astype(I32)
    hub_pick = ones_where(lax.broadcasted_iota(I32, (rows, BLK), 0) == hub_row)

    f_in = w_ref.shape[0]
    loads[2].wait()
    pick = ones_where(
        lax.broadcasted_iota(I32, (BLK, f_in), 1)
        == lax.broadcasted_iota(I32, (BLK, f_in), 0) + j * k_in
    )
    w_mine = dot(pick, w_ref[...])
    w_t = w_mine.T.astype(BF16)[:, :k_in]

    loads[1].wait()
    ft = ft_ref[...]
    hub_ft = dot(ft, hub_pick).astype(BF16)
    hub_part = dot(w_t, hub_ft)
    half = cols // 2
    for d in range(n_feat):
        lower = hub_part[d * cols : d * cols + half]
        upper = hub_part[d * cols + half : (d + 1) * cols]
        hx_out[d] = (lower + pltpu.roll(upper, BLK // 2, 1)).astype(BF16)

    @pl.when(jnp.logical_not(at_desk))
    def _():
        pl.semaphore_wait(barrier, n_feat - 1)

    for desk in desks:

        @pl.when(j == desk - 1)
        def _():
            tell(feat_in, p, desk)

    @pl.when(at_desk)
    def _():
        pl.semaphore_wait(feat_in, 1)

    @pl.when(j == near_desk)
    def _():
        for o in OFFSETS:

            @pl.when(inside(o))
            def _():
                tell(barrier, p + o, near_desk)

        for d in range(1, Y_RING):
            tell(barrier, y_at(d), near_desk)

    @pl.when(j == ring_desk)
    def _():
        for d in range(1, z_ring):
            tell(barrier, z_at(d), ring_desk)

    for d in far_first(n_feat):
        copy = pltpu.make_async_remote_copy(
            src_ref=hx_out.at[feat_at(d)],
            dst_ref=hx.at[d - 1],
            send_sem=hxs,
            recv_sem=hxr,
            device_id={"feat": feat_at(d)},
            device_id_type=MESH,
        )
        copy.start()

    for h in range(n_chunk):
        left = jnp.concatenate(
            [w_t[d * cols + h * chunk : d * cols + (h + 1) * chunk] for d in range(n_feat)], 0
        )
        part = dot(left, ft).astype(BF16)
        for d in range(n_feat):
            sx[d, h] = part[d * chunk : (d + 1) * chunk]
        for d in far_first(n_feat):
            copy = pltpu.make_async_remote_copy(
                src_ref=sx.at[feat_at(d), h],
                dst_ref=rx.at[h, d - 1],
                send_sem=sxs,
                recv_sem=sxr.at[h],
                device_id={"feat": feat_at(d)},
                device_id_type=MESH,
            )
            copy.start()

    loads[3].wait()
    for s in range(slots):
        lo = lax.rem(send_ref[s : s + 1, :], LO)
        hot_ref[s] = ones_where(lax.broadcasted_iota(I32, (LO, halo), 0) == lo)
    @pl.when(j == near_desk)
    def _():
        before_p = lax.min(p, REACH)
        after_p = lax.min(n_dom - 1 - p, REACH)
        pl.semaphore_wait(barrier, before_p + after_p + Y_RING - 1)
        for other in range(n_feat - 1):
            tell(near_in, p, other)

    arrived_in(hx, hxr)
    hub_sum = hx_out[j].astype(F32)
    for d in range(1, n_feat):
        hub_sum = hub_sum + hx[d - 1].astype(F32)
    hub_mine = hub_sum.astype(BF16)
    hub_out[...] = hub_mine
    hy[y] = hub_mine

    @pl.when(j != near_desk)
    def _():
        pl.semaphore_wait(near_in, 1)

    for d in far_first(Y_RING):
        copy = pltpu.make_async_remote_copy(
            src_ref=hub_out,
            dst_ref=hy.at[y],
            send_sem=hys,
            recv_sem=hyr,
            device_id={"dom": y_at(d)},
            device_id_type=MESH,
        )
        copy.start()

    packed = Y_RING * HUB_MOST

    def bulk(h, part=None):
        span = slice(h * chunk, (h + 1) * chunk)
        if part != 1:
            arrived_in(rx.at[h], sxr.at[h])
        total = sx[j, h].astype(F32)
        for d in range(1, n_feat):
            total = total + rx[h, d - 1].astype(F32)
        proj = total.astype(BF16)
        for b in range(0 if part == 1 else own_blocks):
            ext_ref[b, span, :] = proj[:, b * BLK : (b + 1) * BLK]
        stacked = jnp.concatenate([proj[:, g * LO : (g + 1) * LO] for g in range(his)], 0)
        for s in SEND_ORDER if part is None else SEND_ORDER[4 * part : 4 * part + 4]:
            hi = lax.div(send_ref[s : s + 1, :], LO)
            rows_out = pick_groups(dot(stacked, hot_ref[s]), hi, his, chunk).astype(BF16)
            for b in range(slot_blocks):
                sy[h, s, b] = rows_out[:, b * BLK : (b + 1) * BLK]
            first = own_blocks + s * slot_blocks
            copy = pltpu.make_async_remote_copy(
                src_ref=sy.at[h, s],
                dst_ref=ext_ref.at[first : first + slot_blocks, span, :],
                send_sem=sys_.at[s],
                recv_sem=syr.at[s],
                device_id={"dom": p + OFFSETS[s]},
                device_id_type=MESH,
            )

            @pl.when(inside(OFFSETS[s]))
            def _():
                copy.start()

    bulk(0)

    @pl.when(j == ring_desk)
    def _():
        pl.semaphore_wait(barrier, z_ring - 1)
        for other in range(n_feat):
            if other != ring_desk:
                tell(ring_in, p, other)

    bulk(1, 0)

    arrived_in(hy.at[0 : Y_RING - 1], hyr)
    arrived = [hy[source].astype(F32) for source in range(Y_RING)]
    for t in range(packed // BLK):
        lane = lax.broadcasted_iota(I32, (half, BLK), 1) + t * BLK
        low_tile = jnp.zeros((half, BLK), F32)
        high_tile = jnp.zeros((half, BLK), F32)
        for source in range(Y_RING):
            low, high = source * HUB_MOST, (source + 1) * HUB_MOST
            if high <= t * BLK or low >= (t + 1) * BLK:
                continue
            here = (lane >= low) & (lane < high)
            low_tile = jnp.where(here, arrived[source], low_tile)
            high_tile = jnp.where(here, pltpu.roll(arrived[source], BLK // 2, 1), high_tile)
        hpack[:half, t * BLK : (t + 1) * BLK] = low_tile.astype(BF16)
        hpack[half:, t * BLK : (t + 1) * BLK] = high_tile.astype(BF16)
    hz[z] = hpack[...]

    @pl.when(j != ring_desk)
    def _():
        pl.semaphore_wait(ring_in, 1)

    for d in far_first(z_ring):
        copy = pltpu.make_async_remote_copy(
            src_ref=hpack,
            dst_ref=hz.at[z],
            send_sem=hzs,
            recv_sem=hzr,
            device_id={"dom": z_at(d)},
            device_id_type=MESH,
        )
        copy.start()

    bulk(1, 1)
    for h in range(2, n_chunk):
        bulk(h)

    ids_row = as_row(ids)
    owner = lax.div(ids_row, rows)
    owned = lax.broadcasted_iota(I32, (n_dom, hubs), 0) == owner
    earlier = dot(ones_where(owned), ones_where(ascending((hubs, hubs))))
    rank = jnp.sum(jnp.where(owned, earlier, 0.0), 0, keepdims=True).astype(I32)
    end_place = lax.rem(owner, Y_RING) * HUB_MOST + rank
    end_z = lax.div(owner, Y_RING)
    endhot_ref[...] = ones_where(lax.broadcasted_iota(I32, (packed, hubs), 0) == end_place)

    for i in range(4, 8):
        loads[i].wait()
    tiles = meta_in.shape[2]
    live = lax.broadcasted_iota(I32, (1, tiles), 1) < count_in[0]
    meta_ref[0:1, 0:tiles] = jnp.where(live, meta_in[0], own_blocks)
    meta_ref[1:2, 0:tiles] = meta_in[1]
    hand_over = pltpu.make_async_copy(meta_ref, meta_smem, in_sem.at[4])
    hand_over.start()
    eye = lax.broadcasted_iota(I32, (cols, cols), 0) == lax.broadcasted_iota(I32, (cols, cols), 1)
    bias = jnp.sum(jnp.where(eye, bias_in[...], 0.0), 1, keepdims=True)
    bias_ref[...] = jnp.broadcast_to(bias, (cols, BLK))

    for s in range(slots):

        @pl.when(jnp.logical_not(inside(-OFFSETS[s])))
        def _():
            first = own_blocks + s * slot_blocks
            ext_ref[first : first + slot_blocks] = jnp.zeros((slot_blocks, cols, BLK), BF16)

    arrived_in(hz.at[0 : z_ring - 1], hzr)
    everyone = jnp.concatenate([hz[source] for source in range(z_ring)], 0)
    hub_block = pick_groups(dot(everyone, endhot_ref[...]), end_z, z_ring, cols).astype(BF16)
    for b in range(hubs // BLK):
        ext_ref[hub_first + b] = hub_block[:, b * BLK : (b + 1) * BLK]

    loads[8].wait()
    hand_over.wait()
    for s in range(slots):
        first = own_blocks + s * slot_blocks
        slot_rows = ext_ref.at[first : first + slot_blocks]

        @pl.when(inside(-OFFSETS[s]))
        def _():
            arrived_in(slot_rows, syr.at[s])

        @pl.when(inside(OFFSETS[s]))
        def _():
            arrived_in(slot_rows, sys_.at[s])

    arrived_in(hx, hxs)
    arrived_in(rx, sxs)
    arrived_in(hy.at[0 : Y_RING - 1], hys)
    arrived_in(hz.at[0 : z_ring - 1], hzs)


def tile_kernel(meta_ref, tiles_ref, ext_ref, bias_ref, out_ref, acc_ref):
    row_blocks = acc_ref.shape[0] - 1
    acc_ref[...] = jnp.zeros_like(acc_ref)
    unroll = tiles_ref.shape[0]
    columns = ext_ref.shape[1]

    @pl.loop(0, tiles_ref.shape[0] // unroll)
    def _(step):
        products = []
        for u in range(0, unroll, 2):
            t = step * unroll + u
            left = jnp.concatenate([ext_ref[meta_ref[1, t]], ext_ref[meta_ref[1, t + 1]]], 0)
            both = dot(left, tiles_ref[pl.ds(t, 2)].reshape(2 * BLK, BLK), 1, 1)
            products += [both[:columns, :BLK], both[columns:, BLK:]]
        for u in range(unroll):
            acc_ref[meta_ref[0, step * unroll + u]] += products[u]

    bias = bias_ref[...]
    for b in range(row_blocks):
        out_ref[:, b * BLK : (b + 1) * BLK] = jnp.maximum(acc_ref[b] + bias, 0.0).astype(BF16)


def local(
    n_dom, n_feat,
    features, weight, out_bias, tile_values, tile_rows, tile_cols, tile_count, send_rows, hub_ids,
):
    rows, _ = features.shape
    cols = out_bias.shape[0]
    hubs = hub_ids.shape[0]
    slots, halo = send_rows.shape[1:]
    chunk = 8
    n_chunk = cols // chunk
    z_ring = n_dom // Y_RING
    blocks = (rows + slots * halo + hubs) // BLK
    vmem = pl.BlockSpec(memory_space=pltpu.VMEM)
    dma = pltpu.SemaphoreType.DMA
    tiles = tile_values.shape[0]
    shape = jax.ShapeDtypeStruct
    carried = 2 * blocks * cols * BLK + 2 * tile_values.size + 4 * (8 + cols) * BLK
    extended, held_tiles, meta, bias = pl.pallas_call(
        functools.partial(exchange_kernel, n_dom, n_feat, cols, chunk),
        out_shape=(
            pltpu.VMEM((blocks, cols, BLK), BF16),
            pltpu.VMEM(tile_values.shape, BF16),
            pltpu.SMEM((8, BLK), I32),
            pltpu.VMEM((cols, BLK), F32),
        ),
        in_specs=[pl.BlockSpec(memory_space=pltpu.HBM)] * 9,
        out_specs=(vmem, vmem, pl.BlockSpec(memory_space=pltpu.SMEM), vmem),
        scratch_shapes=[
            pltpu.VMEM((features.shape[1], rows), BF16),
            pltpu.VMEM(weight.shape, BF16),
            pltpu.VMEM((slots, halo), I32),
            pltpu.VMEM((hubs // BLK, BLK), I32),
            pltpu.VMEM((slots, LO, halo), BF16),
            pltpu.VMEM((Y_RING * HUB_MOST, hubs), BF16),
            pltpu.VMEM((n_feat, n_chunk, chunk, rows), BF16),
            pltpu.VMEM((n_chunk, n_feat - 1, chunk, rows), BF16),
            pltpu.VMEM((n_chunk, slots, halo // BLK, chunk, BLK), BF16),
            pltpu.VMEM((n_feat, cols // 2, BLK), BF16),
            pltpu.VMEM((n_feat - 1, cols // 2, BLK), BF16),
            pltpu.VMEM((cols // 2, BLK), BF16),
            pltpu.VMEM((Y_RING, cols // 2, BLK), BF16),
            pltpu.VMEM((cols, Y_RING * HUB_MOST), BF16),
            pltpu.VMEM((z_ring, cols, Y_RING * HUB_MOST), BF16),
            pltpu.VMEM((2, 1, tiles), I32),
            pltpu.VMEM((8, BLK), I32),
            pltpu.SMEM((1,), I32),
            pltpu.VMEM((1, cols), F32),
            dma((9,)),
            dma,
            dma((n_chunk,)),
            dma((slots,)),
            dma((slots,)),
            dma,
            dma,
            dma,
            dma,
            dma,
            dma,
            pltpu.SemaphoreType.REGULAR,
            pltpu.SemaphoreType.REGULAR,
            pltpu.SemaphoreType.REGULAR,
        ],
        compiler_params=pltpu.CompilerParams(
            collective_id=0,
            has_side_effects=True,
            vmem_limit_bytes=VMEM_MOST - carried - 65536,
        ),
        name="exchange",
    )(
        features.T, weight, send_rows[0], hub_ids.reshape(hubs // BLK, BLK), tile_values,
        tile_rows[None, :], tile_cols[None, :], tile_count, out_bias[None, :],
    )
    out_t = pl.pallas_call(
        tile_kernel,
        out_shape=shape((cols, rows), BF16),
        in_specs=[pl.BlockSpec(memory_space=pltpu.SMEM), vmem, vmem, vmem],
        out_specs=vmem,
        scratch_shapes=[pltpu.VMEM((rows // BLK + 1, cols, BLK), F32)],
        compiler_params=pltpu.CompilerParams(vmem_limit_bytes=16 * 2**20),
        name="tiles",
    )(meta, held_tiles, extended, bias)
    return out_t.T


def solution(mesh):
    in_specs = (
        P("dom", "feat"),
        P(),
        P("feat"),
        P("dom", None, None),
        P("dom"),
        P("dom"),
        P("dom"),
        P("dom", None, None),
        P(),
    )
    out_specs = P("dom", "feat")
    body = functools.partial(local, mesh.shape["dom"], mesh.shape["feat"])
    return jax.shard_map(body, mesh=mesh, in_specs=in_specs, out_specs=out_specs, check_vma=False)
```

```python
import functools

import jax
import jax.numpy as jnp
from jax import lax
from jax.experimental import pallas as pl
from jax.experimental.pallas import tpu as pltpu
from jax.sharding import PartitionSpec as P

REACH = 4
HUB_MOST = 48
Y_RING = 8
LO = 256
BLK = 128
OFFSETS = tuple(range(-REACH, 0)) + tuple(range(1, REACH + 1))
SEND_ORDER = (0, 7, 1, 6, 2, 5, 3, 4)
VMEM_MOST = 67_043_328
MESH = pl.DeviceIdType.MESH
F32, BF16, I32 = jnp.float32, jnp.bfloat16, jnp.int32


def dims(a, b):
    return (((a,), (b,)), ((), ()))


def dot(a, b, ca=1, cb=0):
    return lax.dot_general(a, b, dims(ca, cb), preferred_element_type=F32)


def ones_where(mask):
    return jnp.where(mask, 1.0, 0.0).astype(BF16)


def ascending(shape, swap=False):
    a, b = lax.broadcasted_iota(I32, shape, 0), lax.broadcasted_iota(I32, shape, 1)
    return b < a if swap else a < b


def pick_groups(stacked, group_of, groups, height):
    total = jnp.zeros((height, stacked.shape[1]), F32)
    for g in range(groups):
        total = jnp.where(group_of == g, stacked[g * height : (g + 1) * height], total)
    return total


def arrived_in(ref, sem):
    pltpu.make_async_copy(ref, ref, sem).wait()


def far_first(ring):
    return sorted(range(1, ring), key=lambda d: -min(d, ring - d))


def as_row(x):
    return jnp.concatenate([x[i : i + 1] for i in range(x.shape[0])], 1)


def exchange_kernel(
    n_dom, n_feat, cols, chunk,
    ft_hbm, w_hbm, send_hbm, hub_hbm, tiles_hbm, rows_hbm, cols_hbm, count_hbm, bias_hbm,
    ext_ref, tiles_ref, meta_smem, bias_ref,
    ft_ref, w_ref, send_ref, hub_ref, hot_ref, endhot_ref, sx, rx, sy,
    hx_out, hx, hub_out, hy, hpack, hz, meta_in, meta_ref, count_in, bias_in,
    in_sem, sxs, sxr, sys_, syr, hxs, hxr, hys, hyr, hzs, hzr, feat_in, near_in, ring_in,
):
    p = lax.axis_index("dom")
    j = lax.axis_index("feat")
    y = lax.rem(p, Y_RING)
    z = lax.div(p, Y_RING)
    z_ring = n_dom // Y_RING
    k_in, rows = ft_ref.shape
    n_chunk = cols // chunk
    his = rows // LO
    slots, halo = send_ref.shape
    own_blocks = rows // BLK
    slot_blocks = halo // BLK
    hub_first = own_blocks + slots * slot_blocks
    near_desk, ring_desk = n_feat - 1, n_feat - 3
    desks = (near_desk, ring_desk)
    at_desk = (j == near_desk) | (j == ring_desk)

    loads = []
    for i, (src, dst) in enumerate(
        (
            (hub_hbm, hub_ref), (ft_hbm, ft_ref), (w_hbm, w_ref), (send_hbm, send_ref),
            (rows_hbm, meta_in.at[0]), (cols_hbm, meta_in.at[1]),
            (count_hbm, count_in), (bias_hbm, bias_in), (tiles_hbm, tiles_ref),
        )
    ):
        loads.append(pltpu.make_async_copy(src, dst, in_sem.at[i]))
        loads[-1].start()

    def y_at(step):
        return z * Y_RING + lax.rem(y + step, Y_RING)

    def z_at(step):
        return lax.rem(z + step, z_ring) * Y_RING + y

    def feat_at(step):
        return lax.rem(j + step, n_feat)

    def tell(sem, dom, feat):
        pl.semaphore_signal(
            sem, inc=1, device_id={"dom": dom, "feat": feat}, device_id_type=MESH
        )

    def inside(o):
        return (p + o >= 0) & (p + o < n_dom)

    barrier = pltpu.get_barrier_semaphore()
    for other in range(n_feat):
        if other in desks:
            continue

        @pl.when(j != other)
        def _():
            tell(barrier, p, other)

    loads[0].wait()

    ids = hub_ref[...]
    hubs = ids.size
    mine = lax.div(ids, rows) == p
    mine_ones = ones_where(mine)
    side = ids.shape[0]
    in_row = dot(mine_ones, ones_where(ascending((BLK, BLK))))
    above = jnp.sum(dot(ones_where(ascending((side, side), True)), mine_ones), 1, keepdims=True)
    my_rank = (in_row + above).astype(I32)
    local_row = lax.rem(ids, rows)
    place = as_row(jnp.where(mine, lax.rem(my_rank + y * HUB_MOST, BLK), -1))
    taken = ones_where(lax.broadcasted_iota(I32, (BLK, hubs), 0) == place)
    halves = jnp.concatenate(
        [as_row(lax.rem(local_row, LO).astype(F32)), as_row((lax.div(local_row, LO) + 1).astype(F32))]
        + [jnp.zeros((14, hubs), F32)],
        0,
    ).astype(BF16)
    listed = dot(halves, taken, 1, 1)
    hub_row = (listed[0:1] + LO * (listed[1:2] - 1.0)).astype(I32)
    hub_pick = ones_where(lax.broadcasted_iota(I32, (rows, BLK), 0) == hub_row)

    f_in = w_ref.shape[0]
    loads[2].wait()
    pick = ones_where(
        lax.broadcasted_iota(I32, (BLK, f_in), 1)
        == lax.broadcasted_iota(I32, (BLK, f_in), 0) + j * k_in
    )
    w_mine = dot(pick, w_ref[...])
    w_t = w_mine.T.astype(BF16)[:, :k_in]

    loads[1].wait()
    ft = ft_ref[...]
    hub_ft = dot(ft, hub_pick).astype(BF16)
    hub_part = dot(w_t, hub_ft)
    half = cols // 2
    for d in range(n_feat):
        lower = hub_part[d * cols : d * cols + half]
        upper = hub_part[d * cols + half : (d + 1) * cols]
        hx_out[d] = (lower + pltpu.roll(upper, BLK // 2, 1)).astype(BF16)

    @pl.when(jnp.logical_not(at_desk))
    def _():
        pl.semaphore_wait(barrier, n_feat - 1)

    for desk in desks:

        @pl.when(j == desk - 1)
        def _():
            tell(feat_in, p, desk)

    @pl.when(at_desk)
    def _():
        pl.semaphore_wait(feat_in, 1)

    @pl.when(j == near_desk)
    def _():
        for o in OFFSETS:

            @pl.when(inside(o))
            def _():
                tell(barrier, p + o, near_desk)

        for d in range(1, Y_RING):
            tell(barrier, y_at(d), near_desk)

    @pl.when(j == ring_desk)
    def _():
        for d in range(1, z_ring):
            tell(barrier, z_at(d), ring_desk)

    for d in far_first(n_feat):
        copy = pltpu.make_async_remote_copy(
            src_ref=hx_out.at[feat_at(d)],
            dst_ref=hx.at[d - 1],
            send_sem=hxs,
            recv_sem=hxr,
            device_id={"feat": feat_at(d)},
            device_id_type=MESH,
        )
        copy.start()

    for h in range(n_chunk):
        left = jnp.concatenate(
            [w_t[d * cols + h * chunk : d * cols + (h + 1) * chunk] for d in range(n_feat)], 0
        )
        part = dot(left, ft).astype(BF16)
        for d in range(n_feat):
            sx[d, h] = part[d * chunk : (d + 1) * chunk]
        for d in far_first(n_feat):
            copy = pltpu.make_async_remote_copy(
                src_ref=sx.at[feat_at(d), h],
                dst_ref=rx.at[h, d - 1],
                send_sem=sxs,
                recv_sem=sxr.at[h],
                device_id={"feat": feat_at(d)},
                device_id_type=MESH,
            )
            copy.start()

    loads[3].wait()
    for s in range(slots):
        lo = lax.rem(send_ref[s : s + 1, :], LO)
        hot_ref[s] = ones_where(lax.broadcasted_iota(I32, (LO, halo), 0) == lo)
    @pl.when(j == near_desk)
    def _():
        before_p = lax.min(p, REACH)
        after_p = lax.min(n_dom - 1 - p, REACH)
        pl.semaphore_wait(barrier, before_p + after_p + Y_RING - 1)
        for other in range(n_feat - 1):
            tell(near_in, p, other)

    arrived_in(hx, hxr)
    hub_sum = hx_out[j].astype(F32)
    for d in range(1, n_feat):
        hub_sum = hub_sum + hx[d - 1].astype(F32)
    hub_mine = hub_sum.astype(BF16)
    hub_out[...] = hub_mine
    hy[y] = hub_mine

    @pl.when(j != near_desk)
    def _():
        pl.semaphore_wait(near_in, 1)

    for d in far_first(Y_RING):
        copy = pltpu.make_async_remote_copy(
            src_ref=hub_out,
            dst_ref=hy.at[y],
            send_sem=hys,
            recv_sem=hyr,
            device_id={"dom": y_at(d)},
            device_id_type=MESH,
        )
        copy.start()

    packed = Y_RING * HUB_MOST

    def bulk(h, part=None):
        span = slice(h * chunk, (h + 1) * chunk)
        if part != 1:
            arrived_in(rx.at[h], sxr.at[h])
        total = sx[j, h].astype(F32)
        for d in range(1, n_feat):
            total = total + rx[h, d - 1].astype(F32)
        proj = total.astype(BF16)
        for b in range(0 if part == 1 else own_blocks):
            ext_ref[b, span, :] = proj[:, b * BLK : (b + 1) * BLK]
        stacked = jnp.concatenate([proj[:, g * LO : (g + 1) * LO] for g in range(his)], 0)
        for s in SEND_ORDER if part is None else SEND_ORDER[4 * part : 4 * part + 4]:
            hi = lax.div(send_ref[s : s + 1, :], LO)
            rows_out = pick_groups(dot(stacked, hot_ref[s]), hi, his, chunk).astype(BF16)
            for b in range(slot_blocks):
                sy[h, s, b] = rows_out[:, b * BLK : (b + 1) * BLK]
            first = own_blocks + s * slot_blocks
            copy = pltpu.make_async_remote_copy(
                src_ref=sy.at[h, s],
                dst_ref=ext_ref.at[first : first + slot_blocks, span, :],
                send_sem=sys_.at[s],
                recv_sem=syr.at[s],
                device_id={"dom": p + OFFSETS[s]},
                device_id_type=MESH,
            )

            @pl.when(inside(OFFSETS[s]))
            def _():
                copy.start()

    bulk(0)

    @pl.when(j == ring_desk)
    def _():
        pl.semaphore_wait(barrier, z_ring - 1)
        for other in range(n_feat):
            if other != ring_desk:
                tell(ring_in, p, other)

    bulk(1, 0)

    arrived_in(hy.at[0 : Y_RING - 1], hyr)
    arrived = [hy[source].astype(F32) for source in range(Y_RING)]
    for t in range(packed // BLK):
        lane = lax.broadcasted_iota(I32, (half, BLK), 1) + t * BLK
        low_tile = jnp.zeros((half, BLK), F32)
        high_tile = jnp.zeros((half, BLK), F32)
        for source in range(Y_RING):
            low, high = source * HUB_MOST, (source + 1) * HUB_MOST
            if high <= t * BLK or low >= (t + 1) * BLK:
                continue
            here = (lane >= low) & (lane < high)
            low_tile = jnp.where(here, arrived[source], low_tile)
            high_tile = jnp.where(here, pltpu.roll(arrived[source], BLK // 2, 1), high_tile)
        hpack[:half, t * BLK : (t + 1) * BLK] = low_tile.astype(BF16)
        hpack[half:, t * BLK : (t + 1) * BLK] = high_tile.astype(BF16)
    hz[z] = hpack[...]

    @pl.when(j != ring_desk)
    def _():
        pl.semaphore_wait(ring_in, 1)

    near_z = [d for d in range(1, z_ring) if min(d, z_ring - d) <= z_ring // 4]
    far_z = [d for d in range(1, z_ring) if d not in near_z]
    for d in far_first(z_ring):
        copy = pltpu.make_async_remote_copy(
            src_ref=hpack,
            dst_ref=hz.at[z],
            send_sem=hzs,
            recv_sem=hzr.at[0 if d in near_z else 1],
            device_id={"dom": z_at(d)},
            device_id_type=MESH,
        )
        copy.start()

    bulk(1, 1)
    for h in range(2, n_chunk):
        bulk(h)

    ids_row = as_row(ids)
    owner = lax.div(ids_row, rows)
    owned = lax.broadcasted_iota(I32, (n_dom, hubs), 0) == owner
    earlier = dot(ones_where(owned), ones_where(ascending((hubs, hubs))))
    rank = jnp.sum(jnp.where(owned, earlier, 0.0), 0, keepdims=True).astype(I32)
    end_place = lax.rem(owner, Y_RING) * HUB_MOST + rank
    end_z = lax.div(owner, Y_RING)
    endhot_ref[...] = ones_where(lax.broadcasted_iota(I32, (packed, hubs), 0) == end_place)

    for i in range(4, 8):
        loads[i].wait()
    tiles = meta_in.shape[2]
    live = lax.broadcasted_iota(I32, (1, tiles), 1) < count_in[0]
    meta_ref[0:1, 0:tiles] = jnp.where(live, meta_in[0], own_blocks)
    meta_ref[1:2, 0:tiles] = meta_in[1]
    hand_over = pltpu.make_async_copy(meta_ref, meta_smem, in_sem.at[4])
    hand_over.start()
    eye = lax.broadcasted_iota(I32, (cols, cols), 0) == lax.broadcasted_iota(I32, (cols, cols), 1)
    bias = jnp.sum(jnp.where(eye, bias_in[...], 0.0), 1, keepdims=True)
    bias_ref[...] = jnp.broadcast_to(bias, (cols, BLK))

    for s in range(slots):

        @pl.when(jnp.logical_not(inside(-OFFSETS[s])))
        def _():
            first = own_blocks + s * slot_blocks
            ext_ref[first : first + slot_blocks] = jnp.zeros((slot_blocks, cols, BLK), BF16)

    hub_block = jnp.zeros((cols, hubs), F32)
    for group, steps in enumerate((near_z, far_z)):
        arrived_in(hz.at[0 : len(steps)], hzr.at[group])
        sources = [lax.rem(z + z_ring - d, z_ring) for d in ([0] if group == 0 else []) + steps]
        found = dot(jnp.concatenate([hz[source] for source in sources], 0), endhot_ref[...])
        for k, source in enumerate(sources):
            hub_block = jnp.where(end_z == source, found[k * cols : (k + 1) * cols], hub_block)
    hub_block = hub_block.astype(BF16)
    for b in range(hubs // BLK):
        ext_ref[hub_first + b] = hub_block[:, b * BLK : (b + 1) * BLK]

    loads[8].wait()
    hand_over.wait()
    for s in range(slots):
        first = own_blocks + s * slot_blocks
        slot_rows = ext_ref.at[first : first + slot_blocks]

        @pl.when(inside(-OFFSETS[s]))
        def _():
            arrived_in(slot_rows, syr.at[s])

        @pl.when(inside(OFFSETS[s]))
        def _():
            arrived_in(slot_rows, sys_.at[s])

    arrived_in(hx, hxs)
    arrived_in(rx, sxs)
    arrived_in(hy.at[0 : Y_RING - 1], hys)
    arrived_in(hz.at[0 : z_ring - 1], hzs)


def tile_kernel(meta_ref, tiles_ref, ext_ref, bias_ref, out_ref, acc_ref):
    row_blocks = acc_ref.shape[0] - 1
    acc_ref[...] = jnp.zeros_like(acc_ref)
    unroll = tiles_ref.shape[0]
    columns = ext_ref.shape[1]

    @pl.loop(0, tiles_ref.shape[0] // unroll)
    def _(step):
        products = []
        for u in range(0, unroll, 2):
            t = step * unroll + u
            left = jnp.concatenate([ext_ref[meta_ref[1, t]], ext_ref[meta_ref[1, t + 1]]], 0)
            both = dot(left, tiles_ref[pl.ds(t, 2)].reshape(2 * BLK, BLK), 1, 1)
            products += [both[:columns, :BLK], both[columns:, BLK:]]
        for u in range(unroll):
            acc_ref[meta_ref[0, step * unroll + u]] += products[u]

    bias = bias_ref[...]
    for b in range(row_blocks):
        out_ref[:, b * BLK : (b + 1) * BLK] = jnp.maximum(acc_ref[b] + bias, 0.0).astype(BF16)


def local(
    n_dom, n_feat,
    features, weight, out_bias, tile_values, tile_rows, tile_cols, tile_count, send_rows, hub_ids,
):
    rows, _ = features.shape
    cols = out_bias.shape[0]
    hubs = hub_ids.shape[0]
    slots, halo = send_rows.shape[1:]
    chunk = 8
    n_chunk = cols // chunk
    z_ring = n_dom // Y_RING
    blocks = (rows + slots * halo + hubs) // BLK
    vmem = pl.BlockSpec(memory_space=pltpu.VMEM)
    dma = pltpu.SemaphoreType.DMA
    tiles = tile_values.shape[0]
    shape = jax.ShapeDtypeStruct
    carried = 2 * blocks * cols * BLK + 2 * tile_values.size + 4 * (8 + cols) * BLK
    extended, held_tiles, meta, bias = pl.pallas_call(
        functools.partial(exchange_kernel, n_dom, n_feat, cols, chunk),
        out_shape=(
            pltpu.VMEM((blocks, cols, BLK), BF16),
            pltpu.VMEM(tile_values.shape, BF16),
            pltpu.SMEM((8, BLK), I32),
            pltpu.VMEM((cols, BLK), F32),
        ),
        in_specs=[pl.BlockSpec(memory_space=pltpu.HBM)] * 9,
        out_specs=(vmem, vmem, pl.BlockSpec(memory_space=pltpu.SMEM), vmem),
        scratch_shapes=[
            pltpu.VMEM((features.shape[1], rows), BF16),
            pltpu.VMEM(weight.shape, BF16),
            pltpu.VMEM((slots, halo), I32),
            pltpu.VMEM((hubs // BLK, BLK), I32),
            pltpu.VMEM((slots, LO, halo), BF16),
            pltpu.VMEM((Y_RING * HUB_MOST, hubs), BF16),
            pltpu.VMEM((n_feat, n_chunk, chunk, rows), BF16),
            pltpu.VMEM((n_chunk, n_feat - 1, chunk, rows), BF16),
            pltpu.VMEM((n_chunk, slots, halo // BLK, chunk, BLK), BF16),
            pltpu.VMEM((n_feat, cols // 2, BLK), BF16),
            pltpu.VMEM((n_feat - 1, cols // 2, BLK), BF16),
            pltpu.VMEM((cols // 2, BLK), BF16),
            pltpu.VMEM((Y_RING, cols // 2, BLK), BF16),
            pltpu.VMEM((cols, Y_RING * HUB_MOST), BF16),
            pltpu.VMEM((z_ring, cols, Y_RING * HUB_MOST), BF16),
            pltpu.VMEM((2, 1, tiles), I32),
            pltpu.VMEM((8, BLK), I32),
            pltpu.SMEM((1,), I32),
            pltpu.VMEM((1, cols), F32),
            dma((9,)),
            dma,
            dma((n_chunk,)),
            dma((slots,)),
            dma((slots,)),
            dma,
            dma,
            dma,
            dma,
            dma,
            dma((2,)),
            pltpu.SemaphoreType.REGULAR,
            pltpu.SemaphoreType.REGULAR,
            pltpu.SemaphoreType.REGULAR,
        ],
        compiler_params=pltpu.CompilerParams(
            collective_id=0,
            has_side_effects=True,
            vmem_limit_bytes=VMEM_MOST - carried - 65536,
        ),
        name="exchange",
    )(
        features.T, weight, send_rows[0], hub_ids.reshape(hubs // BLK, BLK), tile_values,
        tile_rows[None, :], tile_cols[None, :], tile_count, out_bias[None, :],
    )
    out_t = pl.pallas_call(
        tile_kernel,
        out_shape=shape((cols, rows), BF16),
        in_specs=[pl.BlockSpec(memory_space=pltpu.SMEM), vmem, vmem, vmem],
        out_specs=vmem,
        scratch_shapes=[pltpu.VMEM((rows // BLK + 1, cols, BLK), F32)],
        compiler_params=pltpu.CompilerParams(vmem_limit_bytes=16 * 2**20),
        name="tiles",
    )(meta, held_tiles, extended, bias)
    return out_t.T


def solution(mesh):
    in_specs = (
        P("dom", "feat"),
        P(),
        P("feat"),
        P("dom", None, None),
        P("dom"),
        P("dom"),
        P("dom"),
        P("dom", None, None),
        P(),
    )
    out_specs = P("dom", "feat")
    body = functools.partial(local, mesh.shape["dom"], mesh.shape["feat"])
    return jax.shard_map(body, mesh=mesh, in_specs=in_specs, out_specs=out_specs, check_vma=False)
```
